128 devices in a mesh: occ: 8 (over y, core), vir: 16 (over x, z).
Axes of the slice: x: 4, y: 4, z: 4, core: 2. Of those that a mesh axis runs over, the one named last changes fastest.
Arguments:
- amplitudes: bfloat16 [32, 32, 256, 256], P('vir', None, 'occ'), may hold values from -0.0234375 to 0.0234375
- pair_factor: bfloat16 [256, 256, 512], P('vir', 'occ'), may hold values from -1.296875 to 1.296875
- block_factor: bfloat16 [32, 256, 512], P(None, None, ('occ', 'vir')), may hold values from -1.296875 to 1.296875
- cycle_matrix: bfloat16 [8192, 8192], P('occ', 'vir'), may hold values from -0.0625 to 0.0625
- occ_energy: float32 [32], replicated, may hold values from -2 to -0.3
- block_energy: float32 [32], replicated, may hold values from 0.2 to 3
- virt_energy: float32 [256], replicated, may hold values from 0.2 to 3
Outputs:
- update: float32 [1024, 8192], P('occ', 'vir')
The draws below stay inside these ranges and needn't reach their ends.
All inputs are finite; a program needn't handle non-finite values.
Results may differ from the reference program's by a relative error of at most 0.0035.
Values may be sent and summed in bfloat16 or wider, within the bound.
No kernel may reach another device: no remote copies, remote signals or barrier semaphores. Data moves between devices by JAX's collectives and lax.ppermute only.
A program may use at most 128 MiB of HBM per device.

```python
import jax
import jax.numpy as jnp
from jax import lax

O = 32
V = 256
NAUX = 512
VB = 32


def shard_levels(stream_key, dims, shards, low, top_value):
    def one(axis_at, shards_of):
        steps = jax.random.uniform(jax.random.fold_in(jax.random.fold_in(stream_key, 6), axis_at), (shards_of,), jnp.float32, low / len(shards), top_value / len(shards))
        return jnp.repeat(jnp.exp(steps), dims[axis_at] // shards_of).reshape((-1,) + (1,) * (len(dims) - axis_at - 1))

    level = one(*shards[0])
    for cut in shards[1:]:
        level = level * one(*cut)
    return level


def centred(own_key, extent, spread, limit, split=(), held_as=jnp.bfloat16):
    result = spread * jax.random.normal(own_key, extent, jnp.float32)
    if split:
        result = result * shard_levels(own_key, extent, split, -0.22, 0.18)
    return jnp.clip(result, -limit, limit).astype(held_as)


def setup_inputs(seed: int = 0) -> dict:
    splits = jax.random.split(jax.random.key(seed), 8)
    return {
        "amplitudes": centred(splits[0], (O, O, V, V), (V * V) ** -0.5, 0.0234375, ((0, 16), (2, 8))),
        "pair_factor": centred(splits[1], (V, V, NAUX), 0.21, 1.296875, ((0, 16), (1, 8))),
        "block_factor": centred(splits[2], (VB, V, NAUX), 0.21, 1.296875, ((2, 128),)),
        "cycle_matrix": centred(splits[3], (O * V, V * O), (O * V) ** -0.5, 0.0625, ((0, 8), (1, 16))),
        "occ_energy": jnp.clip(jax.random.uniform(splits[4], (O,), jnp.float32, -2.0, -0.3), -2.0, -0.3),
        "block_energy": jnp.clip(jax.random.uniform(splits[5], (VB,), jnp.float32, 0.2, 3.0), 0.2, 3.0),
        "virt_energy": jnp.clip(jax.random.uniform(splits[6], (V,), jnp.float32, 0.2, 3.0), 0.2, 3.0),
    }


def reference(amplitudes, pair_factor, block_factor, cycle_matrix, occ_energy, block_energy, virt_energy):
    stride = 16
    left = block_factor.reshape(VB * V, NAUX)
    widened = amplitudes.astype(jnp.float32)

    def one_block(index):
        rows = lax.dynamic_slice_in_dim(pair_factor, index * stride, stride, 0)
        right = rows.reshape(stride * V, NAUX)
        integral = lax.dot_general(left, right, (((1,), (1,)), ((), ())), preferred_element_type=jnp.float32)
        integral = integral.astype(jnp.bfloat16).reshape(VB, V, stride, V)
        return jnp.einsum("ijdc,acbd->ijab", widened, integral.astype(jnp.float32))

    blocks = lax.map(one_block, jnp.arange(V // stride, dtype=jnp.int32))
    ladder = blocks.transpose(1, 2, 3, 0, 4).reshape(O, O, VB, V)
    holes = ladder.astype(jnp.bfloat16).transpose(0, 2, 1, 3).reshape(O * VB, O * V)
    cycle = jnp.dot(holes, cycle_matrix, preferred_element_type=jnp.float32)
    divisor = (block_energy[None, :, None, None] + virt_energy[None, None, :, None]
               - occ_energy[:, None, None, None] - occ_energy[None, None, None, :])
    residual = ladder.transpose(0, 2, 3, 1).reshape(O * VB, V * O) + cycle
    return residual / divisor.reshape(O * VB, V * O)
```

```python
import functools

import jax
import jax.numpy as jnp
from jax import lax
from jax.experimental import pallas as pl
from jax.experimental.pallas import tpu as pltpu
from jax.sharding import PartitionSpec as P

BF16, F32 = jnp.bfloat16, jnp.float32
OCC, VIR = ("y", "core"), ("x", "z")
ALL_CZ = [(c, z) for c in range(2) for z in range(4)]


def amplitude_route(alpha):
    return [(c * 4 + z, (z // 2) * 4 + 2 * c + ((z % 2) ^ alpha)) for c, z in ALL_CZ]


def factor_route(gamma):
    return [(c * 4 + z, ((z ^ gamma) // 2) * 4 + 2 * c + ((z ^ gamma) % 2)) for c, z in ALL_CZ]


def integrals_kernel(where_ref, pair_ref, block_ref, out_ref):
    slots, nd, nb, naux = pair_ref.shape
    nc = block_ref.shape[3]
    rhs = jnp.concatenate(
        [block_ref[:, k].reshape(naux, nc) for k in range(block_ref.shape[1])], axis=1
    )
    for s in range(slots):
        lhs = pair_ref[where_ref[0] ^ s].reshape(nd * nb, naux)
        got = jnp.dot(lhs, rhs, preferred_element_type=F32).astype(BF16)
        for k in range(block_ref.shape[1]):
            for d in range(nd):
                out_ref[
                    (k * slots + s) * nb : (k * slots + s + 1) * nb, d * nc : (d + 1) * nc
                ] = got[d * nb : (d + 1) * nb, k * nc : (k + 1) * nc]


def form_integrals(where, pair, block):
    slots, nd, nb, naux = pair.shape
    groups, na, nq, nc = block.shape
    step = 2
    return pl.pallas_call(
        integrals_kernel,
        grid_spec=pltpu.PrefetchScalarGridSpec(
            num_scalar_prefetch=1,
            grid=(na // step,),
            in_specs=[
                pl.BlockSpec((slots, nd, nb, naux), lambda g, w: (0, 0, 0, 0)),
                pl.BlockSpec((groups, step, nq, nc), lambda g, w: (0, g, 0, 0)),
            ],
            out_specs=pl.BlockSpec((step * slots * nb, nd * nc), lambda g, w: (g, 0)),
        ),
        out_shape=jax.ShapeDtypeStruct((na * slots * nb, nd * nc), BF16),
        name="integrals",
    )(where, pair, block)


def ladder_kernel(half_ref, amp_ref, w_ref, out_ref, turned):
    nx, two, nd, rows, nc = amp_ref.shape
    wide = two * rows

    @pl.when(pl.program_id(0) == 0)
    def _():
        for x in range(nx):
            for d in range(nd):
                pair = jnp.concatenate(
                    [amp_ref[x, half_ref[0] ^ p, d] for p in range(two)], axis=0
                )
                turned[d * nc : (d + 1) * nc, x * wide : (x + 1) * wide] = pair.T

    got = jnp.dot(w_ref[...], turned[...], preferred_element_type=F32).astype(BF16)
    ny, nz, na, nb, _ = out_ref.shape
    for y in range(ny):
        for z in range(nz):
            for a in range(na):
                row = (a * nz + z) * nb
                out_ref[y, z, a] = got[row : row + nb, y * wide : (y + 1) * wide]


def partial_ladder(half, amp, w, nz):
    nx, two, nd, rows, nc = amp.shape
    nrow, depth = w.shape
    step = 512
    nb = 16
    na = step // (nz * nb)
    return pl.pallas_call(
        ladder_kernel,
        grid_spec=pltpu.PrefetchScalarGridSpec(
            num_scalar_prefetch=1,
            grid=(nrow // step,),
            in_specs=[
                pl.BlockSpec(amp.shape, lambda g, h: (0, 0, 0, 0, 0)),
                pl.BlockSpec((step, depth), lambda g, h: (g, 0)),
            ],
            out_specs=pl.BlockSpec((nx, nz, na, nb, two * rows), lambda g, h: (0, 0, g, 0, 0)),
            scratch_shapes=[pltpu.VMEM((depth, nx * two * rows), BF16)],
        ),
        out_shape=jax.ShapeDtypeStruct((nx, nz, nrow // (nz * nb), nb, two * rows), BF16),
        name="ladder",
    )(half, amp, w)


def settle_kernel(parts_ref, direct_ref, holes_ref, total, swapped):
    peers, rows, wide = parts_ref.shape
    nb = 16
    na = rows // nb
    ni = wide // na
    nj = wide // ni
    acc = parts_ref[0].astype(F32)
    for p in range(1, peers):
        acc = acc + parts_ref[p].astype(F32)
    total[...] = acc
    per = wide // nj
    for group in range(nb // per):
        blocks = [total[pl.ds(group * per + k, na, stride=nb), :] for k in range(per)]
        for i in range(ni):
            direct_ref[i * na : (i + 1) * na, group * wide : (group + 1) * wide] = jnp.concatenate(
                [m[:, i * nj : (i + 1) * nj] for m in blocks], axis=1
            )
        for k, m in enumerate(blocks):
            flipped = m.T
            swapped[pl.ds(group * per + k, nj, stride=nb), :] = jnp.concatenate(
                [flipped[i * nj : (i + 1) * nj, :] for i in range(ni)], axis=1
            )
    holes_ref[...] = swapped[...].astype(BF16)


def settle(parts):
    peers, rows, wide = parts.shape
    return pl.pallas_call(
        settle_kernel,
        out_shape=(
            jax.ShapeDtypeStruct((128, 512), F32),
            jax.ShapeDtypeStruct((rows, wide), BF16),
        ),
        scratch_shapes=[pltpu.VMEM((rows, wide), F32), pltpu.VMEM((rows, wide), F32)],
        name="settle",
    )(parts)


def cycle_kernel(holes_ref, matrix_ref, direct_ref, row_ref, col_ref, out_ref, acc):
    g = pl.program_id(0)
    peers, nk, nb, wide = holes_ref.shape
    lhs = jnp.concatenate(
        [holes_ref[:, k].reshape(peers * nb, wide).T for k in range(nk)], axis=1
    )
    got = jnp.dot(lhs, matrix_ref[...], preferred_element_type=F32)

    @pl.when(g == 0)
    def _():
        acc[...] = direct_ref[...] + got

    @pl.when(g > 0)
    def _():
        acc[...] += got

    @pl.when(g == pl.num_programs(0) - 1)
    def _():
        out_ref[...] = acc[...] / (row_ref[...] + col_ref[...])


def finish(holes, matrix, direct, row, col):
    peers, nk, nb, wide = holes.shape
    depth, ncol = matrix.shape
    step = 4
    return pl.pallas_call(
        cycle_kernel,
        grid=(nk // step,),
        in_specs=[
            pl.BlockSpec((peers, step, nb, wide), lambda g: (0, g, 0, 0)),
            pl.BlockSpec((step * depth // nk, ncol), lambda g: (g, 0)),
            pl.BlockSpec(direct.shape, lambda g: (0, 0)),
            pl.BlockSpec(row.shape, lambda g: (0, 0)),
            pl.BlockSpec(col.shape, lambda g: (0, 0)),
        ],
        out_specs=pl.BlockSpec(direct.shape, lambda g: (0, 0)),
        out_shape=jax.ShapeDtypeStruct(direct.shape, F32),
        scratch_shapes=[pltpu.VMEM(direct.shape, F32)],
        name="cycle",
    )(holes, matrix, direct, row, col)


def on_device(
    amplitudes, pair_factor, block_factor, cycle_matrix, occ_energy, block_energy, virt_energy
):
    y, core, x, z = (lax.axis_index(n) for n in ("y", "core", "x", "z"))
    half = z % 2
    ni, nj, nd, nc = amplitudes.shape
    pieces = amplitudes.reshape(ni * nj, nd, 2, nc // 2).transpose(2, 1, 0, 3)
    got = [
        lax.ppermute(
            lax.dynamic_index_in_dim(pieces, half ^ alpha, 0, keepdims=False),
            ("core", "z"),
            amplitude_route(alpha),
        )
        for alpha in range(2)
    ]
    amp = lax.all_gather(jnp.stack(got), "x", axis=0)

    turned = pair_factor.transpose(1, 0, 2)
    pair = jnp.stack([lax.ppermute(turned, ("core", "z"), factor_route(g)) for g in range(4)])

    block = lax.all_gather(block_factor.transpose(2, 0, 1), VIR, axis=0)
    nv, nq, na, _ = block.shape
    block = lax.dynamic_slice_in_dim(block, half * (nc // 2), nc // 2, 3)
    block = block.reshape(nv * nq, na, nc // 2).transpose(1, 0, 2)
    block = lax.all_gather(block, OCC, axis=0)

    where = (2 * core + half).astype(jnp.int32).reshape(1)
    w = form_integrals(where, pair, block)
    parts = partial_ladder(half.astype(jnp.int32).reshape(1), amp, w, 4)
    parts = parts.reshape(16, *parts.shape[2:])
    parts = lax.all_to_all(parts, ("y", "z"), 0, 0, tiled=True)
    direct, holes = settle(parts.reshape(16, -1, parts.shape[-1]))
    holes = lax.all_gather(holes.reshape(nj, -1, holes.shape[1]), VIR, axis=0)
    matrix = lax.all_gather(cycle_matrix, OCC, axis=0, tiled=True)

    occ_rows = nj // 8
    cols = virt_energy.shape[0] // 16
    occ_here = lax.dynamic_slice_in_dim(occ_energy, (2 * y + core) * occ_rows, occ_rows, 0)
    virt_here = lax.dynamic_slice_in_dim(virt_energy, (4 * x + z) * cols, cols, 0)
    row = (block_energy[None, :] - occ_here[:, None]).reshape(-1, 1)
    col = (virt_here[:, None] - occ_energy[None, :]).reshape(1, -1)
    return finish(holes, matrix, direct, row, col)


def solution(mesh):
    fine = jax.sharding.Mesh(mesh.devices.reshape(4, 2, 4, 4), ("y", "core", "x", "z"))
    return jax.shard_map(
        on_device,
        mesh=fine,
        in_specs=(
            P(VIR, None, OCC, None),
            P(VIR, OCC, None),
            P(None, None, OCC + VIR),
            P(OCC, VIR),
            P(),
            P(),
            P(),
        ),
        out_specs=P(OCC, VIR),
        check_vma=False,
    )
```

```python
import functools

import jax
import jax.numpy as jnp
from jax import lax
from jax.experimental import pallas as pl
from jax.experimental.pallas import tpu as pltpu
from jax.sharding import PartitionSpec as P

BF16, F32 = jnp.bfloat16, jnp.float32
OCC, VIR = ("y", "core"), ("x", "z")
ALL_CZ = [(c, z) for c in range(2) for z in range(4)]


def amplitude_route(alpha):
    return [(c * 4 + z, (z // 2) * 4 + 2 * c + ((z % 2) ^ alpha)) for c, z in ALL_CZ]


def ring(value, axis, shift):
    n = lax.axis_size(axis)
    return lax.ppermute(value, axis, [(i, (i + shift) % n) for i in range(n)])


def sibling(value):
    return lax.ppermute(value, "core", [(0, 1), (1, 0)])


def integrals_kernel(where_ref, *refs):
    pairs, blocks, out_ref, rhs = refs[:4], refs[4:8], refs[8], refs[9]
    nd, nb, naux = pairs[0].shape
    two, nq, nc = blocks[0].shape
    for far, ref in enumerate(blocks):
        start = pl.multiple_of(((where_ref[0] + 4 - far) % 4) * nq, nq)
        for k in range(two):
            rhs[pl.ds(start, nq), k * nc : (k + 1) * nc] = ref[k]
    for s, ref in enumerate(pairs):
        got = jnp.dot(
            ref[...].reshape(nd * nb, naux), rhs[...], preferred_element_type=F32
        ).astype(BF16)
        for k in range(two):
            for d in range(nd):
                out_ref[(k * 4 + s) * nb : (k * 4 + s + 1) * nb, d * nc : (d + 1) * nc] = got[
                    d * nb : (d + 1) * nb, k * nc : (k + 1) * nc
                ]


def form_integrals(where, pairs, blocks):
    nd, nb, naux = pairs[0].shape
    na, nq, nc = blocks[0].shape
    step = 2
    return pl.pallas_call(
        integrals_kernel,
        grid_spec=pltpu.PrefetchScalarGridSpec(
            num_scalar_prefetch=1,
            grid=(na // step,),
            in_specs=[pl.BlockSpec((nd, nb, naux), lambda g, w: (0, 0, 0))] * 4
            + [pl.BlockSpec((step, nq, nc), lambda g, w: (g, 0, 0))] * 4,
            out_specs=pl.BlockSpec((step * 4 * nb, nd * nc), lambda g, w: (g, 0)),
            scratch_shapes=[pltpu.VMEM((naux, step * nc), BF16)],
        ),
        out_shape=jax.ShapeDtypeStruct((na * 4 * nb, nd * nc), BF16),
        name="integrals",
    )(where, *pairs, *blocks)


SHIFTS = (0, 3, 1, 2)


def ladder_kernel(where_ref, *refs):
    amps, w_ref, out_ref, turned = refs[:16], refs[16], refs[17], refs[18]
    nd, rows, nc = amps[0].shape
    wide = 2 * rows

    @pl.when(pl.program_id(0) == 0)
    def _():
        flip = where_ref[2] == 1
        for n in range(8):
            first, second = amps[2 * n], amps[2 * n + 1]
            for d in range(nd):
                p, q = first[d], second[d]
                pair = jnp.concatenate([jnp.where(flip, q, p), jnp.where(flip, p, q)], axis=0)
                turned[d * nc : (d + 1) * nc, n * wide : (n + 1) * wide] = pair.T

    got = jnp.dot(w_ref[...], turned[...], preferred_element_type=F32).astype(BF16)
    ny, two, nz, na, nb, _ = out_ref.shape
    for n in range(8):
        y = (where_ref[0] + SHIFTS[n // 2]) % 4
        c = where_ref[1] ^ (n % 2)
        for s in range(nz):
            for a in range(na):
                row = (a * nz + s) * nb
                out_ref[y, c, where_ref[3] ^ s, a] = got[row : row + nb, n * wide : (n + 1) * wide]


def partial_ladder(where, amps, w):
    nd, rows, nc = amps[0].shape
    nrow, depth = w.shape
    step, nz, nb = 256, 4, 16
    na = step // (nz * nb)
    return pl.pallas_call(
        ladder_kernel,
        grid_spec=pltpu.PrefetchScalarGridSpec(
            num_scalar_prefetch=1,
            grid=(nrow // step,),
            in_specs=[pl.BlockSpec((nd, rows, nc), lambda g, h: (0, 0, 0))] * 16
            + [pl.BlockSpec((step, depth), lambda g, h: (g, 0))],
            out_specs=pl.BlockSpec((4, 2, nz, na, nb, 2 * rows), lambda g, h: (0, 0, 0, g, 0, 0)),
            scratch_shapes=[pltpu.VMEM((depth, 16 * rows), BF16)],
        ),
        out_shape=jax.ShapeDtypeStruct((4, 2, nz, nrow // (nz * nb), nb, 2 * rows), BF16),
        name="ladder",
    )(where, *amps, w)


def settle_kernel(parts_ref, direct_ref, holes_ref, total, swapped):
    ny, two, nz, part, wide = parts_ref.shape
    rows = two * part
    nb = 16
    na = rows // nb
    ni = wide // na
    nj = wide // ni
    for h in range(two):
        acc = parts_ref[0, h, 0].astype(F32)
        for p in range(1, ny * nz):
            acc = acc + parts_ref[p // nz, h, p % nz].astype(F32)
        total[h * part : (h + 1) * part] = acc
    per = wide // nj
    for group in range(nb // per):
        blocks = [total[pl.ds(group * per + k, na, stride=nb), :] for k in range(per)]
        for i in range(ni):
            direct_ref[i * na : (i + 1) * na, group * wide : (group + 1) * wide] = jnp.concatenate(
                [m[:, i * nj : (i + 1) * nj] for m in blocks], axis=1
            )
        for k, m in enumerate(blocks):
            flipped = m.T
            swapped[pl.ds(group * per + k, nj, stride=nb), :] = jnp.concatenate(
                [flipped[i * nj : (i + 1) * nj, :] for i in range(ni)], axis=1
            )
    holes_ref[...] = swapped[...].astype(BF16)


def settle(parts):
    rows, wide = parts.shape[1] * parts.shape[3], parts.shape[4]
    return pl.pallas_call(
        settle_kernel,
        out_shape=(
            jax.ShapeDtypeStruct((128, 512), F32),
            jax.ShapeDtypeStruct((rows, wide), BF16),
        ),
        scratch_shapes=[pltpu.VMEM((rows, wide), F32), pltpu.VMEM((rows, wide), F32)],
        name="settle",
    )(parts)


def cycle_kernel(where_ref, holes_ref, *refs):
    pieces, (direct_ref, row_ref, col_ref, out_ref) = refs[:10], refs[10:]
    peers, _, nb, wide = holes_ref.shape
    acc = direct_ref[...]
    chunks = [(s, side, n * 2 + side, 0, 4) for n, s in enumerate((0, 3, 1)) for side in (0, 1)]
    chunks += [(2, side, 6 + 2 * part + side, 2 * part, 2) for part in (0, 1) for side in (0, 1)]
    for shift, side, at, base, count in chunks:
        owner = ((where_ref[0] + shift) % 4) * 2 + (where_ref[1] ^ side)
        lhs = jnp.concatenate(
            [
                holes_ref[:, owner * 4 + base + k].reshape(peers * nb, wide).T
                for k in range(count)
            ],
            axis=1,
        )
        acc = acc + jnp.dot(lhs, pieces[at][...], preferred_element_type=F32)
    out_ref[...] = acc / (row_ref[...] + col_ref[...])


def finish(where, holes, pieces, direct, row, col):
    return pl.pallas_call(
        cycle_kernel,
        in_specs=[pl.BlockSpec(memory_space=pltpu.SMEM)]
        + [pl.BlockSpec(memory_space=pltpu.VMEM)] * (len(pieces) + 4),
        out_specs=pl.BlockSpec(memory_space=pltpu.VMEM),
        out_shape=jax.ShapeDtypeStruct(direct.shape, F32),
        name="cycle",
    )(where, holes, *pieces, direct, row, col)


def on_device(
    amplitudes, pair_factor, block_factor, cycle_matrix, occ_energy, block_energy, virt_energy
):
    y, core, x, z = (lax.axis_index(n) for n in ("y", "core", "x", "z"))
    half = z % 2
    ni, nj, nd, nc = amplitudes.shape
    pieces = amplitudes.reshape(ni * nj, nd, 2, nc // 2).transpose(2, 1, 0, 3)
    own = [
        lax.ppermute(
            lax.dynamic_index_in_dim(pieces, half ^ alpha, 0, keepdims=False),
            ("core", "z"),
            amplitude_route(alpha),
        )
        for alpha in range(2)
    ]
    left = [ring(v, "x", 1) for v in own]
    right = [ring(v, "x", -1) for v in own]
    far = [ring(left[0], "x", 1), ring(right[1], "x", -1)]
    amps = []
    for pair in (own, left, right, far):
        amps += pair + [sibling(v) for v in pair]

    turned = pair_factor.transpose(1, 0, 2)
    pair = [lax.ppermute(turned, ("core", "z"), amplitude_route(alpha)) for alpha in range(2)]
    pair += [sibling(v) for v in pair]

    na, _, nq = block_factor.shape
    block = block_factor.reshape(2, na // 2, 2, nc // 2, nq).transpose(0, 2, 1, 4, 3)
    block = jnp.broadcast_to(block[:, None, None], (2, 4, 2, 2, na // 2, nq, nc // 2))
    block = lax.all_to_all(
        block.reshape(32, na // 2, nq, nc // 2), ("core", "x", "z"), 0, 0, tiled=True
    )
    block = block.transpose(1, 0, 2, 3).reshape(na // 2, 32 * nq, nc // 2)
    blocks = [block] + [ring(block, "y", k) for k in (1, 2, 3)]

    before, after = ring(cycle_matrix, "y", 1), ring(cycle_matrix, "y", -1)
    mid = cycle_matrix.shape[0] // 2
    matrix = []
    for v in (cycle_matrix, before, after, ring(before[:mid], "y", 1), ring(after[mid:], "y", -1)):
        matrix += [v, sibling(v)]

    def scalars(*values):
        return jnp.stack([jnp.asarray(v, jnp.int32) for v in values])

    w = form_integrals(scalars(y), pair, blocks)
    parts = partial_ladder(scalars(x, core, half, 2 * core + half), amps, w)
    parts = parts.reshape(32, -1, parts.shape[-1])
    parts = lax.all_to_all(parts, ("y", "core", "z"), 0, 0, tiled=True)
    direct, holes = settle(parts.reshape(4, 2, 4, -1, parts.shape[-1]))
    holes = jnp.broadcast_to(holes.reshape(1, nj, -1, holes.shape[1]), (16, nj, 16, 128))
    holes = lax.all_to_all(holes, VIR, 0, 0, tiled=True)

    occ_rows = nj // 8
    cols = virt_energy.shape[0] // 16
    occ_here = lax.dynamic_slice_in_dim(occ_energy, (2 * y + core) * occ_rows, occ_rows, 0)
    virt_here = lax.dynamic_slice_in_dim(virt_energy, (4 * x + z) * cols, cols, 0)
    row = (block_energy[None, :] - occ_here[:, None]).reshape(-1, 1)
    col = (virt_here[:, None] - occ_energy[None, :]).reshape(1, -1)
    return finish(scalars(y, core), holes, matrix, direct, row, col)


def solution(mesh):
    fine = jax.sharding.Mesh(mesh.devices.reshape(4, 2, 4, 4), ("y", "core", "x", "z"))
    return jax.shard_map(
        on_device,
        mesh=fine,
        in_specs=(
            P(VIR, None, OCC, None),
            P(VIR, OCC, None),
            P(None, None, OCC + VIR),
            P(OCC, VIR),
            P(),
            P(),
            P(),
        ),
        out_specs=P(OCC, VIR),
        check_vma=False,
    )
```

```python
import functools

import jax
import jax.numpy as jnp
from jax import lax
from jax.experimental import pallas as pl
from jax.experimental.pallas import tpu as pltpu
from jax.sharding import PartitionSpec as P

BF16, F32 = jnp.bfloat16, jnp.float32
OCC, VIR = ("y", "core"), ("x", "z")
ALL_CZ = [(c, z) for c in range(2) for z in range(4)]


def amplitude_route(alpha):
    return [(c * 4 + z, (z // 2) * 4 + 2 * c + ((z % 2) ^ alpha)) for c, z in ALL_CZ]


def ring(value, axis, shift):
    n = lax.axis_size(axis)
    return lax.ppermute(value, axis, [(i, (i + shift) % n) for i in range(n)])


def sibling(value):
    return lax.ppermute(value, "core", [(0, 1), (1, 0)])


def integrals_kernel(where_ref, *refs):
    pairs, blocks, out_ref, rhs = refs[:4], refs[4:8], refs[8], refs[9]
    nd, nb, naux = pairs[0].shape
    two, nq, nc = blocks[0].shape
    for far, ref in enumerate(blocks):
        start = pl.multiple_of(((where_ref[0] + 4 - far) % 4) * nq, nq)
        for k in range(two):
            rhs[pl.ds(start, nq), k * nc : (k + 1) * nc] = ref[k]
    for s, ref in enumerate(pairs):
        got = jnp.dot(
            ref[...].reshape(nd * nb, naux), rhs[...], preferred_element_type=F32
        ).astype(BF16)
        for k in range(two):
            for d in range(nd):
                out_ref[(k * 4 + s) * nb : (k * 4 + s + 1) * nb, d * nc : (d + 1) * nc] = got[
                    d * nb : (d + 1) * nb, k * nc : (k + 1) * nc
                ]


def form_integrals(where, pairs, blocks):
    nd, nb, naux = pairs[0].shape
    na, nq, nc = blocks[0].shape
    step = 2
    return pl.pallas_call(
        integrals_kernel,
        grid_spec=pltpu.PrefetchScalarGridSpec(
            num_scalar_prefetch=1,
            grid=(na // step,),
            in_specs=[pl.BlockSpec((nd, nb, naux), lambda g, w: (0, 0, 0))] * 4
            + [pl.BlockSpec((step, nq, nc), lambda g, w: (g, 0, 0))] * 4,
            out_specs=pl.BlockSpec((step * 4 * nb, nd * nc), lambda g, w: (g, 0)),
            scratch_shapes=[pltpu.VMEM((naux, step * nc), BF16)],
        ),
        out_shape=jax.ShapeDtypeStruct((na * 4 * nb, nd * nc), BF16),
        cost_estimate=pl.CostEstimate(
            flops=8 * nd * nb * naux * na * nc, bytes_accessed=12 << 20, transcendentals=0
        ),
        name="integrals",
    )(where, *pairs, *blocks)


def ladder_kernel(aliased, where_ref, *refs):
    at_w = len(refs) - (3 if not aliased else 4)
    amps, w_ref, out_ref, turned = refs[:at_w], refs[at_w], refs[-2], refs[-1]
    _, nd, rows, nc = amps[0].shape
    wide = 2 * rows
    j = pl.program_id(1)

    @pl.when((pl.program_id(0) == 0) & (j == 0))
    def _():
        flip = where_ref[3]
        for n in range(4):
            at = n % 2 * wide
            if n < 2 or len(amps) == 4:
                whole = amps[n]
                read = lambda k, d: whole[flip ^ k, d]
            else:
                first, second = amps[n], amps[n + 2]
                read = lambda k, d: jnp.where((flip ^ k) == 1, second[0, d], first[0, d])
            for d in range(nd):
                pair = jnp.concatenate([read(0, d), read(1, d)], axis=0)
                turned[n // 2, d * nc : (d + 1) * nc, at : at + wide] = pair.T

    got = jnp.dot(w_ref[...], turned[j], preferred_element_type=F32).astype(BF16)
    _, two, nz, na, nb, _ = out_ref.shape
    for side in range(two):
        c = where_ref[2] ^ side
        for s in range(nz):
            for a in range(na):
                row = (a * nz + s) * nb
                out_ref[0, c, where_ref[4] ^ s, a] = got[
                    row : row + nb, side * wide : (side + 1) * wide
                ]


def partial_ladder(where, amps, w, held=None):
    _, nd, rows, nc = amps[0].shape
    nrow, depth = w.shape
    step, nz, nb = 512, 4, 16
    na = step // (nz * nb)
    more = () if held is None else (held,)
    return pl.pallas_call(
        functools.partial(ladder_kernel, bool(more)),
        grid_spec=pltpu.PrefetchScalarGridSpec(
            num_scalar_prefetch=1,
            grid=(nrow // step, 2),
            in_specs=[pl.BlockSpec(v.shape, lambda g, j, h: (0, 0, 0, 0)) for v in amps]
            + [pl.BlockSpec((step, depth), lambda g, j, h: (g, 0))]
            + [pl.BlockSpec(memory_space=pl.ANY)] * len(more),
            out_specs=pl.BlockSpec(
                (1, 2, nz, na, nb, 2 * rows), lambda g, j, h: (h[j], 0, 0, g, 0, 0)
            ),
            scratch_shapes=[pltpu.VMEM((2, depth, 4 * rows), BF16)],
        ),
        out_shape=jax.ShapeDtypeStruct((4, 2, nz, nrow // (nz * nb), nb, 2 * rows), BF16),
        input_output_aliases={len(amps) + 2: 0} if more else {},
        cost_estimate=pl.CostEstimate(
            flops=2 * nrow * depth * 8 * rows, bytes_accessed=12 << 20, transcendentals=0
        ),
        name="ladder",
    )(where, *amps, w, *more)


def settle_kernel(parts_ref, direct_ref, holes_ref, total, swapped):
    ny, two, nz, part, wide = parts_ref.shape
    rows = two * part
    nb = 16
    na = rows // nb
    ni = wide // na
    nj = wide // ni
    for h in range(two):
        acc = parts_ref[0, h, 0].astype(F32)
        for p in range(1, ny * nz):
            acc = acc + parts_ref[p // nz, h, p % nz].astype(F32)
        total[h * part : (h + 1) * part] = acc
    per = wide // nj
    for group in range(nb // per):
        blocks = [total[pl.ds(group * per + k, na, stride=nb), :] for k in range(per)]
        for i in range(ni):
            direct_ref[i * na : (i + 1) * na, group * wide : (group + 1) * wide] = jnp.concatenate(
                [m[:, i * nj : (i + 1) * nj] for m in blocks], axis=1
            )
        for k, m in enumerate(blocks):
            flipped = m.T
            swapped[pl.ds(group * per + k, nj, stride=nb), :] = jnp.concatenate(
                [flipped[i * nj : (i + 1) * nj, :] for i in range(ni)], axis=1
            )
    held = swapped[...].astype(BF16)
    for p in range(holes_ref.shape[0]):
        holes_ref[p] = held


def settle(parts):
    rows, wide = parts.shape[1] * parts.shape[3], parts.shape[4]
    return pl.pallas_call(
        settle_kernel,
        out_shape=(
            jax.ShapeDtypeStruct((128, 512), F32),
            jax.ShapeDtypeStruct((16, rows, wide), BF16),
        ),
        scratch_shapes=[pltpu.VMEM((rows, wide), F32), pltpu.VMEM((rows, wide), F32)],
        name="settle",
    )(parts)


def cycle_kernel(where_ref, holes_ref, *refs):
    pieces, (direct_ref, row_ref, col_ref, out_ref) = refs[:10], refs[10:]
    peers, _, nb, wide = holes_ref.shape
    acc = direct_ref[...]
    chunks = [(s, side, n * 2 + side, 0, 4) for n, s in enumerate((0, 3, 1)) for side in (0, 1)]
    chunks += [(2, side, 6 + 2 * part + side, 2 * part, 2) for part in (0, 1) for side in (0, 1)]
    for shift, side, at, base, count in chunks:
        owner = ((where_ref[0] + shift) % 4) * 2 + (where_ref[1] ^ side)
        lhs = jnp.concatenate(
            [
                holes_ref[:, owner * 4 + base + k].reshape(peers * nb, wide).T
                for k in range(count)
            ],
            axis=1,
        )
        acc = acc + jnp.dot(lhs, pieces[at][...], preferred_element_type=F32)
    out_ref[...] = acc / (row_ref[...] + col_ref[...])


def finish(where, holes, pieces, direct, row, col):
    return pl.pallas_call(
        cycle_kernel,
        in_specs=[pl.BlockSpec(memory_space=pltpu.SMEM)]
        + [pl.BlockSpec(memory_space=pltpu.VMEM)] * (len(pieces) + 4),
        out_specs=pl.BlockSpec(memory_space=pltpu.VMEM),
        out_shape=jax.ShapeDtypeStruct(direct.shape, F32),
        name="cycle",
    )(where, holes, *pieces, direct, row, col)


def on_device(
    amplitudes, pair_factor, block_factor, cycle_matrix, occ_energy, block_energy, virt_energy
):
    y, core, x, z = (lax.axis_index(n) for n in ("y", "core", "x", "z"))
    half = z % 2
    ni, nj, nd, nc = amplitudes.shape
    before, after = ring(cycle_matrix, "y", 1), ring(cycle_matrix, "y", -1)

    flat = amplitudes.reshape(ni * nj, nd, nc)
    own = [
        lax.ppermute(
            lax.dynamic_slice_in_dim(flat, (half ^ alpha) * (nc // 2), nc // 2, 2).transpose(1, 0, 2),
            ("core", "z"),
            amplitude_route(alpha),
        )
        for alpha in range(2)
    ]

    na, _, nq = block_factor.shape
    block = block_factor.reshape(2, na // 2, 2, nc // 2, nq).transpose(0, 2, 1, 4, 3)
    block = jnp.broadcast_to(block[:, None, None], (2, 4, 2, 2, na // 2, nq, nc // 2))
    block = lax.all_to_all(
        block.reshape(32, na // 2, nq, nc // 2), ("core", "x", "z"), 0, 0, tiled=True
    )
    block = block.transpose(1, 0, 2, 3).reshape(na // 2, 32 * nq, nc // 2)

    turned = pair_factor.transpose(1, 0, 2)
    *own, turned, block = lax.optimization_barrier((*own, turned, block))
    own = jnp.stack(own)
    left, right = ring(own, "x", 1), ring(own, "x", -1)
    pair = [lax.ppermute(turned, ("core", "z"), amplitude_route(alpha)) for alpha in range(2)]
    far = [ring(left[:1], "x", 1), ring(right[1:], "x", -1)]

    blocks = [block] + [ring(block, "y", k) for k in (1, 2, 3)]
    pair += [sibling(v) for v in pair]
    near = [own, sibling(own), left, sibling(left)]
    rest = [right, sibling(right), far[0], sibling(far[0]), far[1], sibling(far[1])]

    def scalars(*values):
        return jnp.stack([jnp.asarray(v, jnp.int32) for v in values])

    before, after, *blocks = lax.optimization_barrier((before, after, *blocks))
    w = form_integrals(scalars(y), pair, blocks)

    mid = cycle_matrix.shape[0] // 2
    matrix = []
    for v in (cycle_matrix, before, after, ring(before[:mid], "y", 1), ring(after[mid:], "y", -1)):
        matrix += [v, sibling(v)]
    w, *matrix = lax.optimization_barrier((w, *matrix))

    def spots(*shifts):
        return scalars(*[(x + k) % 4 for k in shifts], core, half, 2 * core + half)

    parts = partial_ladder(spots(0, 3), near, w)
    parts = partial_ladder(spots(1, 2), rest, w, parts)
    parts = parts.reshape(32, -1, parts.shape[-1])
    parts = lax.all_to_all(parts, ("y", "core", "z"), 0, 0, tiled=True)
    direct, holes = settle(parts.reshape(4, 2, 4, -1, parts.shape[-1]))
    holes = lax.all_to_all(holes.reshape(16, nj, 16, 128), VIR, 0, 0, tiled=True)

    occ_rows = nj // 8
    cols = virt_energy.shape[0] // 16
    occ_here = lax.dynamic_slice_in_dim(occ_energy, (2 * y + core) * occ_rows, occ_rows, 0)
    virt_here = lax.dynamic_slice_in_dim(virt_energy, (4 * x + z) * cols, cols, 0)
    row = (block_energy[None, :] - occ_here[:, None]).reshape(-1, 1)
    col = (virt_here[:, None] - occ_energy[None, :]).reshape(1, -1)
    return finish(scalars(y, core), holes, matrix, direct, row, col)


def solution(mesh):
    fine = jax.sharding.Mesh(mesh.devices.reshape(4, 2, 4, 4), ("y", "core", "x", "z"))
    return jax.shard_map(
        on_device,
        mesh=fine,
        in_specs=(
            P(VIR, None, OCC, None),
            P(VIR, OCC, None),
            P(None, None, OCC + VIR),
            P(OCC, VIR),
            P(),
            P(),
            P(),
        ),
        out_specs=P(OCC, VIR),
        check_vma=False,
    )
```

```python
import jax
import jax.numpy as jnp
from jax import lax
from jax.experimental import pallas as pl
from jax.experimental.pallas import tpu as pltpu
from jax.sharding import PartitionSpec as P


BF16, F32 = jnp.bfloat16, jnp.float32
OCC, VIR = ("y", "core"), ("x", "z")
ALL_CZ = [(c, z) for c in range(2) for z in range(4)]


def amplitude_route(alpha):
    return [(c * 4 + z, (z // 2) * 4 + 2 * c + ((z % 2) ^ alpha)) for c, z in ALL_CZ]


def ring(value, axis, shift):
    n = lax.axis_size(axis)
    return lax.ppermute(value, axis, [(i, (i + shift) % n) for i in range(n)])


def sibling(value):
    return lax.ppermute(value, "core", [(0, 1), (1, 0)])


def integrals_kernel(where_ref, *refs):
    pairs, blocks, out_ref, rhs = refs[:4], refs[4:8], refs[8], refs[9]
    nd, nb, naux = pairs[0].shape
    two, nq, nc = blocks[0].shape
    for far, ref in zip((0, 1, 3, 2), blocks):
        start = pl.multiple_of(((where_ref[0] + 4 - far) % 4) * nq, nq)
        for k in range(two):
            rhs[pl.ds(start, nq), k * nc : (k + 1) * nc] = ref[k]
    for s, ref in enumerate(pairs):
        got = jnp.dot(
            ref[...].reshape(nd * nb, naux), rhs[...], preferred_element_type=F32
        ).astype(BF16)
        for k in range(two):
            for d in range(nd):
                out_ref[(k * 4 + s) * nb : (k * 4 + s + 1) * nb, d * nc : (d + 1) * nc] = got[
                    d * nb : (d + 1) * nb, k * nc : (k + 1) * nc
                ]


def form_integrals(where, pairs, blocks):
    nd, nb, naux = pairs[0].shape
    na, nq, nc = blocks[0].shape
    step = 2
    return pl.pallas_call(
        integrals_kernel,
        grid_spec=pltpu.PrefetchScalarGridSpec(
            num_scalar_prefetch=1,
            grid=(na // step,),
            in_specs=[pl.BlockSpec((nd, nb, naux), lambda g, w: (0, 0, 0))] * 4
            + [pl.BlockSpec((step, nq, nc), lambda g, w: (g, 0, 0))] * 4,
            out_specs=pl.BlockSpec((step * 4 * nb, nd * nc), lambda g, w: (g, 0)),
            scratch_shapes=[pltpu.VMEM((naux, step * nc), BF16)],
        ),
        out_shape=jax.ShapeDtypeStruct((na * 4 * nb, nd * nc), BF16),
        cost_estimate=pl.CostEstimate(
            flops=8 * nd * nb * naux * na * nc, bytes_accessed=12 << 20, transcendentals=0
        ),
        name="integrals",
    )(where, *pairs, *blocks)


def turn_kernel(where_ref, zero_ref, one_ref, out_ref):
    nd, _, nc = zero_ref.shape
    flip = where_ref[0] == 1
    for d in range(nd):
        p, q = zero_ref[d], one_ref[d]
        pair = jnp.concatenate([jnp.where(flip, q, p), jnp.where(flip, p, q)], axis=0)
        out_ref[d * nc : (d + 1) * nc, :] = pair.T


def turn(where, zero, one):
    nd, rows, nc = zero.shape
    return pl.pallas_call(
        turn_kernel,
        in_specs=[pl.BlockSpec(memory_space=pltpu.SMEM)]
        + [pl.BlockSpec(memory_space=pltpu.VMEM)] * 2,
        out_specs=pl.BlockSpec(memory_space=pltpu.VMEM),
        out_shape=jax.ShapeDtypeStruct((nd * nc, 2 * rows), BF16),
        name="turn",
    )(where, zero, one)


def ladder_kernel(where_ref, *refs):
    amps, w_ref, out_ref, turned = refs[:-3], refs[-3], refs[-2], refs[-1]
    depth, wide = amps[0].shape
    j = pl.program_id(1)

    @pl.when((pl.program_id(0) == 0) & (j == 0))
    def _():
        for n in range(6):
            at = n % 2 * wide
            turned[n // 2, :, at : at + wide] = amps[n][...]
        for n in range(4):
            at = n % 2 * wide
            row = n // 2 * (depth // 2)
            turned[3, row : row + depth // 2, at : at + wide] = amps[6 + n][...]

    got = jnp.dot(w_ref[...], turned[j], preferred_element_type=F32).astype(BF16)
    _, two, nz, na, nb, _ = out_ref.shape
    for side in range(two):
        c = where_ref[4] ^ side
        for s in range(nz):
            for a in range(na):
                row = (a * nz + s) * nb
                out_ref[0, c, where_ref[5] ^ s, a] = got[
                    row : row + nb, side * wide : (side + 1) * wide
                ]


def partial_ladder(where, amps, w):
    wide = amps[0].shape[1]
    nrow, depth = w.shape
    step, nz, nb = 512, 4, 16
    na = step // (nz * nb)
    return pl.pallas_call(
        ladder_kernel,
        grid_spec=pltpu.PrefetchScalarGridSpec(
            num_scalar_prefetch=1,
            grid=(nrow // step, 4),
            in_specs=[pl.BlockSpec(v.shape, lambda g, j, h: (0, 0)) for v in amps]
            + [pl.BlockSpec((step, depth), lambda g, j, h: (g, 0))],
            out_specs=pl.BlockSpec(
                (1, 2, nz, na, nb, wide), lambda g, j, h: (h[j], 0, 0, g, 0, 0)
            ),
            scratch_shapes=[pltpu.VMEM((4, depth, 2 * wide), BF16)],
        ),
        out_shape=jax.ShapeDtypeStruct((4, 2, nz, nrow // (nz * nb), nb, wide), BF16),
        cost_estimate=pl.CostEstimate(
            flops=16 * nrow * depth * wide, bytes_accessed=18 << 20, transcendentals=0
        ),
        name="ladder",
    )(where, *amps, w)


def settle_kernel(parts_ref, direct_ref, holes_ref, total, swapped):
    ny, two, nz, part, wide = parts_ref.shape
    rows = two * part
    nb = 16
    na = rows // nb
    ni = wide // na
    nj = wide // ni
    for h in range(two):
        acc = parts_ref[0, h, 0].astype(F32)
        for p in range(1, ny * nz):
            acc = acc + parts_ref[p // nz, h, p % nz].astype(F32)
        total[h * part : (h + 1) * part] = acc
    per = wide // nj
    for group in range(nb // per):
        blocks = [total[pl.ds(group * per + k, na, stride=nb), :] for k in range(per)]
        for i in range(ni):
            direct_ref[i * na : (i + 1) * na, group * wide : (group + 1) * wide] = jnp.concatenate(
                [m[:, i * nj : (i + 1) * nj] for m in blocks], axis=1
            )
        for k, m in enumerate(blocks):
            flipped = m.T
            swapped[pl.ds(group * per + k, nj, stride=nb), :] = jnp.concatenate(
                [flipped[i * nj : (i + 1) * nj, :] for i in range(ni)], axis=1
            )
    held = swapped[...].astype(BF16)
    for p in range(holes_ref.shape[0]):
        holes_ref[p] = held


def settle(parts):
    rows, wide = parts.shape[1] * parts.shape[3], parts.shape[4]
    return pl.pallas_call(
        settle_kernel,
        out_shape=(
            jax.ShapeDtypeStruct((128, 512), F32),
            jax.ShapeDtypeStruct((16, rows, wide), BF16),
        ),
        scratch_shapes=[pltpu.VMEM((rows, wide), F32), pltpu.VMEM((rows, wide), F32)],
        name="settle",
    )(parts)


def cycle_kernel(where_ref, holes_ref, *refs):
    pieces, (direct_ref, row_ref, col_ref, out_ref) = refs[:10], refs[10:]
    peers, _, nb, wide = holes_ref.shape
    acc = direct_ref[...]
    chunks = [(s, side, n * 2 + side, 0, 4) for n, s in enumerate((0, 3, 1)) for side in (0, 1)]
    chunks += [(2, side, 6 + 2 * part + side, 2 * part, 2) for part in (0, 1) for side in (0, 1)]
    for shift, side, at, base, count in chunks:
        owner = ((where_ref[0] + shift) % 4) * 2 + (where_ref[1] ^ side)
        lhs = jnp.concatenate(
            [
                holes_ref[:, owner * 4 + base + k].reshape(peers * nb, wide).T
                for k in range(count)
            ],
            axis=1,
        )
        acc = acc + jnp.dot(lhs, pieces[at][...], preferred_element_type=F32)
    out_ref[...] = acc / (row_ref[...] + col_ref[...])


def finish(where, holes, pieces, direct, row, col):
    return pl.pallas_call(
        cycle_kernel,
        in_specs=[pl.BlockSpec(memory_space=pltpu.SMEM)]
        + [pl.BlockSpec(memory_space=pltpu.VMEM)] * (len(pieces) + 4),
        out_specs=pl.BlockSpec(memory_space=pltpu.VMEM),
        out_shape=jax.ShapeDtypeStruct(direct.shape, F32),
        name="cycle",
    )(where, holes, *pieces, direct, row, col)


def update(
    amplitudes, pair_factor, block_factor, cycle_matrix, occ_energy, block_energy, virt_energy
):
    y, core, x, z = (lax.axis_index(n) for n in ("y", "core", "x", "z"))
    half = z % 2
    ni, nj, nd, nc = amplitudes.shape

    def scalars(*values):
        return jnp.stack([jnp.asarray(v, jnp.int32) for v in values])

    na, _, nq = block_factor.shape
    block = block_factor.reshape(2, na // 2, 2, nc // 2, nq).transpose(0, 2, 1, 4, 3)
    block = jnp.broadcast_to(block[:, None, None], (2, 4, 2, 2, na // 2, nq, nc // 2))
    block = lax.all_to_all(
        block.reshape(32, na // 2, nq, nc // 2), ("core", "x", "z"), 0, 0, tiled=True
    )
    block = block.transpose(1, 0, 2, 3).reshape(na // 2, 32 * nq, nc // 2)

    flat = amplitudes.reshape(ni * nj, nd, nc)
    own = [
        lax.ppermute(
            lax.dynamic_slice_in_dim(flat, (half ^ alpha) * (nc // 2), nc // 2, 2).transpose(
                1, 0, 2
            ),
            ("core", "z"),
            amplitude_route(alpha),
        )
        for alpha in range(2)
    ]
    own = turn(scalars(half), *own)

    left, right = ring(own, "x", 1), ring(own, "x", -1)
    blocks = [block] + [ring(block, "y", k) for k in (1, 3, 2)]
    turned = pair_factor.transpose(1, 0, 2)
    turned, own = lax.optimization_barrier((turned, own))
    pair = [lax.ppermute(turned, ("core", "z"), amplitude_route(alpha)) for alpha in range(2)]
    before, after = ring(cycle_matrix, "y", 1), ring(cycle_matrix, "y", -1)

    left, right, *blocks = lax.optimization_barrier((left, right, *blocks))
    mid = own.shape[0] // 2
    far = [ring(left[:mid], "x", 1), ring(right[mid:], "x", -1)]
    pair += [sibling(v) for v in pair]
    amps = []
    for v in (own, left, right):
        amps += [v, sibling(v)]
    for v in far:
        amps += [v, sibling(v)]

    w = form_integrals(scalars(y), pair, blocks)
    w, before, after = lax.optimization_barrier((w, before, after))

    spots = scalars(x, (x + 3) % 4, (x + 1) % 4, (x + 2) % 4, core, 2 * core + half)
    parts = partial_ladder(spots, amps, w)
    parts = parts.reshape(32, -1, parts.shape[-1])
    parts = lax.all_to_all(parts, ("y", "core", "z"), 0, 0, tiled=True)
    direct, holes = settle(parts.reshape(4, 2, 4, -1, parts.shape[-1]))
    holes = lax.all_to_all(holes.reshape(16, nj, 16, 128), VIR, 0, 0, tiled=True)

    mid = cycle_matrix.shape[0] // 2
    matrix = []
    ends = ring(before[:mid], "y", 1), ring(after[mid:], "y", -1)
    for v in (cycle_matrix, before, after, *ends):
        matrix += [v, sibling(v)]

    occ_rows = nj // 8
    cols = virt_energy.shape[0] // 16
    occ_here = lax.dynamic_slice_in_dim(occ_energy, (2 * y + core) * occ_rows, occ_rows, 0)
    virt_here = lax.dynamic_slice_in_dim(virt_energy, (4 * x + z) * cols, cols, 0)
    row = (block_energy[None, :] - occ_here[:, None]).reshape(-1, 1)
    col = (virt_here[:, None] - occ_energy[None, :]).reshape(1, -1)
    return finish(scalars(y, core), holes, matrix, direct, row, col)


def solution(mesh):
    fine = jax.sharding.Mesh(mesh.devices.reshape(4, 2, 4, 4), ("y", "core", "x", "z"))
    return jax.shard_map(
        update,
        mesh=fine,
        in_specs=(
            P(VIR, None, OCC, None),
            P(VIR, OCC, None),
            P(None, None, OCC + VIR),
            P(OCC, VIR),
            P(),
            P(),
            P(),
        ),
        out_specs=P(OCC, VIR),
        check_vma=False,
    )
```

```python
import jax
import jax.numpy as jnp
from jax import lax
from jax.experimental import pallas as pl
from jax.experimental.pallas import tpu as pltpu
from jax.sharding import PartitionSpec as P


BF16, F32 = jnp.bfloat16, jnp.float32
OCC, VIR = ("y", "core"), ("x", "z")
ALL_CZ = [(c, z) for c in range(2) for z in range(4)]


def amplitude_route(alpha):
    return [(c * 4 + z, (z // 2) * 4 + 2 * c + ((z % 2) ^ alpha)) for c, z in ALL_CZ]


def ring(value, axis, shift):
    n = lax.axis_size(axis)
    return lax.ppermute(value, axis, [(i, (i + shift) % n) for i in range(n)])


def sibling(value):
    return lax.ppermute(value, "core", [(0, 1), (1, 0)])


def integrals_kernel(where_ref, *refs):
    pairs, blocks, out_ref, rhs = refs[:4], refs[4:8], refs[8], refs[9]
    nd, nb, naux = pairs[0].shape
    two, nq, nc = blocks[0].shape
    for far, ref in zip((0, 1, 3, 2), blocks):
        start = pl.multiple_of(((where_ref[0] + 4 - far) % 4) * nq, nq)
        for k in range(two):
            rhs[pl.ds(start, nq), k * nc : (k + 1) * nc] = ref[k]
    for s, ref in enumerate(pairs):
        got = jnp.dot(
            ref[...].reshape(nd * nb, naux), rhs[...], preferred_element_type=F32
        ).astype(BF16)
        for k in range(two):
            for d in range(nd):
                out_ref[(k * 4 + s) * nb : (k * 4 + s + 1) * nb, d * nc : (d + 1) * nc] = got[
                    d * nb : (d + 1) * nb, k * nc : (k + 1) * nc
                ]


def form_integrals(where, pairs, blocks, part, parts):
    nd, nb, naux = pairs[0].shape
    na, nq, nc = blocks[0].shape
    na, step = na // parts, 2
    skip = part * na // step
    return pl.pallas_call(
        integrals_kernel,
        grid_spec=pltpu.PrefetchScalarGridSpec(
            num_scalar_prefetch=1,
            grid=(na // step,),
            in_specs=[pl.BlockSpec((nd, nb, naux), lambda g, w: (0, 0, 0))] * 4
            + [pl.BlockSpec((step, nq, nc), lambda g, w: (g + skip, 0, 0))] * 4,
            out_specs=pl.BlockSpec((step * 4 * nb, nd * nc), lambda g, w: (g, 0)),
            scratch_shapes=[pltpu.VMEM((naux, step * nc), BF16)],
        ),
        out_shape=jax.ShapeDtypeStruct((na * 4 * nb, nd * nc), BF16),
        cost_estimate=pl.CostEstimate(
            flops=8 * nd * nb * naux * na * nc, bytes_accessed=12 << 20, transcendentals=0
        ),
        name="integrals",
    )(where, *pairs, *blocks)


def turn_kernel(where_ref, zero_ref, one_ref, out_ref):
    nd, _, nc = zero_ref.shape
    flip = where_ref[0] == 1
    for d in range(nd):
        p, q = zero_ref[d], one_ref[d]
        pair = jnp.concatenate([jnp.where(flip, q, p), jnp.where(flip, p, q)], axis=0)
        out_ref[d * nc : (d + 1) * nc, :] = pair.T


def turn(where, zero, one):
    nd, rows, nc = zero.shape
    return pl.pallas_call(
        turn_kernel,
        in_specs=[pl.BlockSpec(memory_space=pltpu.SMEM)]
        + [pl.BlockSpec(memory_space=pltpu.VMEM)] * 2,
        out_specs=pl.BlockSpec(memory_space=pltpu.VMEM),
        out_shape=jax.ShapeDtypeStruct((nd * nc, 2 * rows), BF16),
        name="turn",
    )(where, zero, one)


def ladder_kernel(where_ref, *refs):
    amps, w_ref, out_ref, turned, sems = refs[:-4], refs[-4], refs[-3], refs[-2], refs[-1]
    depth, wide = amps[0].shape
    g, j = pl.program_id(0), pl.program_id(1)

    def load(n):
        at = pl.ds(n % 2 * wide, wide)
        if n < 6:
            spot = turned.at[n // 2, :, at]
        else:
            spot = turned.at[3, pl.ds((n - 6) // 2 * (depth // 2), depth // 2), at]
        return pltpu.make_async_copy(amps[n], spot, sems.at[n])

    @pl.when((g == 0) & (j == 0))
    def _():
        for n in range(10):
            load(n).start()

    for chunk in range(4):

        @pl.when((g == 0) & (j == chunk))
        def _():
            for n in (2 * chunk, 2 * chunk + 1) if chunk < 3 else range(6, 10):
                load(n).wait()

    got = jnp.dot(w_ref[...], turned[j], preferred_element_type=F32).astype(BF16)
    _, two, nz, na, nb, _ = out_ref.shape
    for side in range(two):
        c = where_ref[4] ^ side
        for s in range(nz):
            for a in range(na):
                row = (a * nz + s) * nb
                out_ref[0, c, where_ref[5] ^ s, a] = got[
                    row : row + nb, side * wide : (side + 1) * wide
                ]


def partial_ladder(where, amps, w):
    wide = amps[0].shape[1]
    nrow, depth = w.shape
    step, nz, nb = 256, 4, 16
    na = step // (nz * nb)
    return pl.pallas_call(
        ladder_kernel,
        grid_spec=pltpu.PrefetchScalarGridSpec(
            num_scalar_prefetch=1,
            grid=(nrow // step, 4),
            in_specs=[pl.BlockSpec(memory_space=pl.ANY) for _ in amps]
            + [pl.BlockSpec((step, depth), lambda g, j, h: (g, 0))],
            out_specs=pl.BlockSpec(
                (1, 2, nz, na, nb, wide), lambda g, j, h: (h[j], 0, 0, g, 0, 0)
            ),
            scratch_shapes=[
                pltpu.VMEM((4, depth, 2 * wide), BF16),
                pltpu.SemaphoreType.DMA((len(amps),)),
            ],
        ),
        out_shape=jax.ShapeDtypeStruct((4, 2, nz, nrow // (nz * nb), nb, wide), BF16),
        cost_estimate=pl.CostEstimate(
            flops=16 * nrow * depth * wide, bytes_accessed=14 << 20, transcendentals=0
        ),
        name="ladder",
    )(where, *amps, w)


def settle_kernel(first_ref, second_ref, direct_ref, holes_ref, total, swapped):
    ny, two, nz, part, wide = first_ref.shape
    rows = 2 * two * part
    nb = 16
    na = rows // nb
    ni = wide // na
    nj = wide // ni
    for n in range(2 * two):
        h, ref = n // 2, (first_ref, second_ref)[n % 2]
        acc = ref[0, h, 0].astype(F32)
        for p in range(1, ny * nz):
            acc = acc + ref[p // nz, h, p % nz].astype(F32)
        total[n * part : (n + 1) * part] = acc
    per = wide // nj
    for group in range(nb // per):
        blocks = [total[pl.ds(group * per + k, na, stride=nb), :] for k in range(per)]
        for i in range(ni):
            direct_ref[i * na : (i + 1) * na, group * wide : (group + 1) * wide] = jnp.concatenate(
                [m[:, i * nj : (i + 1) * nj] for m in blocks], axis=1
            )
        for k, m in enumerate(blocks):
            flipped = m.T
            swapped[pl.ds(group * per + k, nj, stride=nb), :] = jnp.concatenate(
                [flipped[i * nj : (i + 1) * nj, :] for i in range(ni)], axis=1
            )
    held = swapped[...].astype(BF16)
    for p in range(holes_ref.shape[0]):
        holes_ref[p] = held


def settle(first, second):
    rows, wide = 2 * first.shape[1] * first.shape[3], first.shape[4]
    return pl.pallas_call(
        settle_kernel,
        out_shape=(
            jax.ShapeDtypeStruct((128, 512), F32),
            jax.ShapeDtypeStruct((16, rows, wide), BF16),
        ),
        scratch_shapes=[pltpu.VMEM((rows, wide), F32), pltpu.VMEM((rows, wide), F32)],
        name="settle",
    )(first, second)


def cycle_kernel(where_ref, holes_ref, *refs):
    pieces, (direct_ref, row_ref, col_ref, out_ref) = refs[:10], refs[10:]
    peers, _, nb, wide = holes_ref.shape
    acc = direct_ref[...]
    chunks = [(s, side, n * 2 + side, 0, 4) for n, s in enumerate((0, 3, 1)) for side in (0, 1)]
    chunks += [(2, side, 6 + 2 * part + side, 2 * part, 2) for part in (0, 1) for side in (0, 1)]
    for shift, side, at, base, count in chunks:
        owner = ((where_ref[0] + shift) % 4) * 2 + (where_ref[1] ^ side)
        lhs = jnp.concatenate(
            [
                holes_ref[:, owner * 4 + base + k].reshape(peers * nb, wide).T
                for k in range(count)
            ],
            axis=1,
        )
        acc = acc + jnp.dot(lhs, pieces[at][...], preferred_element_type=F32)
    out_ref[...] = acc / (row_ref[...] + col_ref[...])


def finish(where, holes, pieces, direct, row, col):
    return pl.pallas_call(
        cycle_kernel,
        in_specs=[pl.BlockSpec(memory_space=pltpu.SMEM)]
        + [pl.BlockSpec(memory_space=pltpu.VMEM)] * (len(pieces) + 4),
        out_specs=pl.BlockSpec(memory_space=pltpu.VMEM),
        out_shape=jax.ShapeDtypeStruct(direct.shape, F32),
        name="cycle",
    )(where, holes, *pieces, direct, row, col)


def update(
    amplitudes, pair_factor, block_factor, cycle_matrix, occ_energy, block_energy, virt_energy
):
    y, core, x, z = (lax.axis_index(n) for n in ("y", "core", "x", "z"))
    half = z % 2
    ni, nj, nd, nc = amplitudes.shape

    def scalars(*values):
        return jnp.stack([jnp.asarray(v, jnp.int32) for v in values])

    na, _, nq = block_factor.shape
    block = block_factor.reshape(2, na // 2, 2, nc // 2, nq).transpose(0, 2, 1, 4, 3)
    block = jnp.broadcast_to(block[:, None, None], (2, 4, 2, 2, na // 2, nq, nc // 2))
    block = lax.all_to_all(
        block.reshape(32, na // 2, nq, nc // 2), ("core", "x", "z"), 0, 0, tiled=True
    )
    block = block.transpose(1, 0, 2, 3).reshape(na // 2, 32 * nq, nc // 2)

    flat = amplitudes.reshape(ni * nj, nd, nc)
    own = [
        lax.ppermute(
            lax.dynamic_slice_in_dim(flat, (half ^ alpha) * (nc // 2), nc // 2, 2).transpose(
                1, 0, 2
            ),
            ("core", "z"),
            amplitude_route(alpha),
        )
        for alpha in range(2)
    ]
    own = turn(scalars(half), *own)

    left, right = ring(own, "x", 1), ring(own, "x", -1)
    blocks = [block] + [ring(block, "y", k) for k in (1, 3, 2)]
    turned = pair_factor.transpose(1, 0, 2)
    turned, own = lax.optimization_barrier((turned, own))
    pair = [lax.ppermute(turned, ("core", "z"), amplitude_route(alpha)) for alpha in range(2)]
    before, after = ring(cycle_matrix, "y", 1), ring(cycle_matrix, "y", -1)

    left, right, *blocks = lax.optimization_barrier((left, right, *blocks))
    mid = own.shape[0] // 2
    far = [ring(left[:mid], "x", 1), ring(right[mid:], "x", -1)]
    pair += [sibling(v) for v in pair]
    amps = [own, sibling(own)]
    for v in (left, right, *far):
        amps += [v, sibling(v)]

    w = form_integrals(scalars(y), pair, blocks, 0, 2)
    w, before, after = lax.optimization_barrier((w, before, after))

    spots = scalars(x, (x + 3) % 4, (x + 1) % 4, (x + 2) % 4, core, 2 * core + half)

    def exchanged(parts):
        parts = parts.reshape(32, -1, parts.shape[-1])
        parts = lax.all_to_all(parts, ("y", "core", "z"), 0, 0, tiled=True)
        return parts.reshape(4, 2, 4, -1, parts.shape[-1])

    first = exchanged(partial_ladder(spots, amps, w))
    w = form_integrals(scalars(y), pair, blocks, 1, 2)
    second = exchanged(partial_ladder(spots, amps, w))
    direct, holes = settle(first, second)
    holes = lax.all_to_all(holes.reshape(16, nj, 16, 128), VIR, 0, 0, tiled=True)

    mid = cycle_matrix.shape[0] // 2
    matrix = []
    ends = ring(before[:mid], "y", 1), ring(after[mid:], "y", -1)
    for v in (cycle_matrix, before, after, *ends):
        matrix += [v, sibling(v)]

    occ_rows = nj // 8
    cols = virt_energy.shape[0] // 16
    occ_here = lax.dynamic_slice_in_dim(occ_energy, (2 * y + core) * occ_rows, occ_rows, 0)
    virt_here = lax.dynamic_slice_in_dim(virt_energy, (4 * x + z) * cols, cols, 0)
    row = (block_energy[None, :] - occ_here[:, None]).reshape(-1, 1)
    col = (virt_here[:, None] - occ_energy[None, :]).reshape(1, -1)
    return finish(scalars(y, core), holes, matrix, direct, row, col)


def solution(mesh):
    fine = jax.sharding.Mesh(mesh.devices.reshape(4, 2, 4, 4), ("y", "core", "x", "z"))
    return jax.shard_map(
        update,
        mesh=fine,
        in_specs=(
            P(VIR, None, OCC, None),
            P(VIR, OCC, None),
            P(None, None, OCC + VIR),
            P(OCC, VIR),
            P(),
            P(),
            P(),
        ),
        out_specs=P(OCC, VIR),
        check_vma=False,
    )
```

```python
import jax
import jax.numpy as jnp
from jax import lax
from jax.experimental import pallas as pl
from jax.experimental.pallas import tpu as pltpu
from jax.sharding import PartitionSpec as P


BF16, F32 = jnp.bfloat16, jnp.float32
OCC, VIR = ("y", "core"), ("x", "z")
ALL_CZ = [(c, z) for c in range(2) for z in range(4)]


def amplitude_route(alpha):
    return [(c * 4 + z, (z // 2) * 4 + 2 * c + ((z % 2) ^ alpha)) for c, z in ALL_CZ]


def ring(value, axis, shift):
    n = lax.axis_size(axis)
    return lax.ppermute(value, axis, [(i, (i + shift) % n) for i in range(n)])


def sibling(value):
    return lax.ppermute(value, "core", [(0, 1), (1, 0)])


def integrals_kernel(where_ref, *refs):
    pairs, blocks, out_ref, rhs = refs[:4], refs[4:8], refs[8], refs[9]
    nd, nb, naux = pairs[0].shape
    two, nq, nc = blocks[0].shape
    for far, ref in zip((0, 1, 3, 2), blocks):
        start = pl.multiple_of(((where_ref[0] + 4 - far) % 4) * nq, nq)
        for k in range(two):
            rhs[pl.ds(start, nq), k * nc : (k + 1) * nc] = ref[k]
    for s, ref in enumerate(pairs):
        got = jnp.dot(
            ref[...].reshape(nd * nb, naux), rhs[...], preferred_element_type=F32
        ).astype(BF16)
        for k in range(two):
            for d in range(nd):
                out_ref[(k * 4 + s) * nb : (k * 4 + s + 1) * nb, d * nc : (d + 1) * nc] = got[
                    d * nb : (d + 1) * nb, k * nc : (k + 1) * nc
                ]


def form_integrals(where, pairs, blocks):
    nd, nb, naux = pairs[0].shape
    na, nq, nc = blocks[0].shape
    step = 2
    return pl.pallas_call(
        integrals_kernel,
        grid_spec=pltpu.PrefetchScalarGridSpec(
            num_scalar_prefetch=1,
            grid=(na // step,),
            in_specs=[pl.BlockSpec((nd, nb, naux), lambda g, w: (0, 0, 0))] * 4
            + [pl.BlockSpec((step, nq, nc), lambda g, w: (g, 0, 0))] * 4,
            out_specs=pl.BlockSpec((step * 4 * nb, nd * nc), lambda g, w: (g, 0)),
            scratch_shapes=[pltpu.VMEM((naux, step * nc), BF16)],
        ),
        out_shape=jax.ShapeDtypeStruct((na * 4 * nb, nd * nc), BF16),
        cost_estimate=pl.CostEstimate(
            flops=8 * nd * nb * naux * na * nc, bytes_accessed=12 << 20, transcendentals=0
        ),
        name="integrals",
    )(where, *pairs, *blocks)


def turn_kernel(where_ref, zero_ref, one_ref, *out_refs):
    nd, _, nc = zero_ref.shape
    flip = where_ref[0] == 1
    for d in range(nd):
        p, q = zero_ref[d], one_ref[d]
        pair = jnp.concatenate([jnp.where(flip, q, p), jnp.where(flip, p, q)], axis=0)
        at = d % (nd // 2) * nc
        out_refs[d // (nd // 2)][at : at + nc, :] = pair.T


def turn(where, zero, one):
    nd, rows, nc = zero.shape
    return pl.pallas_call(
        turn_kernel,
        in_specs=[pl.BlockSpec(memory_space=pltpu.SMEM)]
        + [pl.BlockSpec(memory_space=pltpu.VMEM)] * 2,
        out_specs=[pl.BlockSpec(memory_space=pltpu.VMEM)] * 2,
        out_shape=[jax.ShapeDtypeStruct((nd * nc // 2, 2 * rows), BF16)] * 2,
        name="turn",
    )(where, zero, one)


def ladder_kernel(where_ref, *refs):
    amps, w_ref, out_ref, turned, sems = refs[:16], refs[16], refs[17], refs[18], refs[19]
    depth, wide = amps[0].shape
    g = pl.program_id(0)

    def load(n):
        chunk, part, side = n // 4, n // 2 % 2, n % 2
        spot = turned.at[pl.ds(part * depth, depth), pl.ds((2 * chunk + side) * wide, wide)]
        return pltpu.make_async_copy(amps[n], spot, sems.at[n])

    @pl.when(g == 0)
    def _():
        for n in range(16):
            load(n).start()

    _, _, nz, na, nb, _ = out_ref.shape
    for part in range(2):

        @pl.when(g == 0)
        def _():
            for n in range(8 * part, 8 * part + 8):
                load(n).wait()

        got = jnp.dot(
            w_ref[...],
            turned[:, 4 * part * wide : 4 * (part + 1) * wide],
            preferred_element_type=F32,
        ).astype(BF16)
        for n in range(4):
            y = where_ref[2 * part + n // 2]
            c = where_ref[4] ^ (n % 2)
            for s in range(nz):
                for a in range(na):
                    row = (a * nz + s) * nb
                    out_ref[y, c, where_ref[5] ^ s, a] = got[
                        row : row + nb, n * wide : (n + 1) * wide
                    ]


def partial_ladder(where, amps, w):
    wide = amps[0].shape[1]
    nrow, depth = w.shape
    step, nz, nb = 512, 4, 16
    na = step // (nz * nb)
    return pl.pallas_call(
        ladder_kernel,
        grid_spec=pltpu.PrefetchScalarGridSpec(
            num_scalar_prefetch=1,
            grid=(nrow // step,),
            in_specs=[pl.BlockSpec(memory_space=pl.ANY) for _ in amps]
            + [pl.BlockSpec((step, depth), lambda g, h: (g, 0))],
            out_specs=pl.BlockSpec((4, 2, nz, na, nb, wide), lambda g, h: (0, 0, 0, g, 0, 0)),
            scratch_shapes=[
                pltpu.VMEM((depth, 8 * wide), BF16),
                pltpu.SemaphoreType.DMA((len(amps),)),
            ],
        ),
        out_shape=jax.ShapeDtypeStruct((4, 2, nz, nrow // (nz * nb), nb, wide), BF16),
        cost_estimate=pl.CostEstimate(
            flops=16 * nrow * depth * wide, bytes_accessed=18 << 20, transcendentals=0
        ),
        name="ladder",
    )(where, *amps, w)


def settle_kernel(parts_ref, direct_ref, holes_ref, total, swapped):
    ny, two, nz, part, wide = parts_ref.shape
    rows = two * part
    nb = 16
    na = rows // nb
    ni = wide // na
    nj = wide // ni
    for h in range(two):
        acc = parts_ref[0, h, 0].astype(F32)
        for p in range(1, ny * nz):
            acc = acc + parts_ref[p // nz, h, p % nz].astype(F32)
        total[h * part : (h + 1) * part] = acc
    per = wide // nj
    for group in range(nb // per):
        blocks = [total[pl.ds(group * per + k, na, stride=nb), :] for k in range(per)]
        for i in range(ni):
            direct_ref[i * na : (i + 1) * na, group * wide : (group + 1) * wide] = jnp.concatenate(
                [m[:, i * nj : (i + 1) * nj] for m in blocks], axis=1
            )
        for k, m in enumerate(blocks):
            flipped = m.T
            swapped[pl.ds(group * per + k, nj, stride=nb), :] = jnp.concatenate(
                [flipped[i * nj : (i + 1) * nj, :] for i in range(ni)], axis=1
            )
    held = swapped[...].astype(BF16)
    for p in range(holes_ref.shape[0]):
        holes_ref[p] = held


def settle(parts):
    rows, wide = parts.shape[1] * parts.shape[3], parts.shape[4]
    return pl.pallas_call(
        settle_kernel,
        out_shape=(
            jax.ShapeDtypeStruct((128, 512), F32),
            jax.ShapeDtypeStruct((16, rows, wide), BF16),
        ),
        scratch_shapes=[pltpu.VMEM((rows, wide), F32), pltpu.VMEM((rows, wide), F32)],
        name="settle",
    )(parts)


def cycle_kernel(where_ref, holes_ref, *refs):
    pieces, (direct_ref, row_ref, col_ref, out_ref) = refs[:10], refs[10:]
    peers, _, nb, wide = holes_ref.shape
    acc = direct_ref[...]
    chunks = [(s, side, n * 2 + side, 0, 4) for n, s in enumerate((0, 3, 1)) for side in (0, 1)]
    chunks += [(2, side, 6 + 2 * part + side, 2 * part, 2) for part in (0, 1) for side in (0, 1)]
    for shift, side, at, base, count in chunks:
        owner = ((where_ref[0] + shift) % 4) * 2 + (where_ref[1] ^ side)
        lhs = jnp.concatenate(
            [
                holes_ref[:, owner * 4 + base + k].reshape(peers * nb, wide).T
                for k in range(count)
            ],
            axis=1,
        )
        acc = acc + jnp.dot(lhs, pieces[at][...], preferred_element_type=F32)
    out_ref[...] = acc / (row_ref[...] + col_ref[...])


def finish(where, holes, pieces, direct, row, col):
    return pl.pallas_call(
        cycle_kernel,
        in_specs=[pl.BlockSpec(memory_space=pltpu.SMEM)]
        + [pl.BlockSpec(memory_space=pltpu.VMEM)] * (len(pieces) + 4),
        out_specs=pl.BlockSpec(memory_space=pltpu.VMEM),
        out_shape=jax.ShapeDtypeStruct(direct.shape, F32),
        name="cycle",
    )(where, holes, *pieces, direct, row, col)


def update(
    amplitudes, pair_factor, block_factor, cycle_matrix, occ_energy, block_energy, virt_energy
):
    y, core, x, z = (lax.axis_index(n) for n in ("y", "core", "x", "z"))
    half = z % 2
    ni, nj, nd, nc = amplitudes.shape

    def scalars(*values):
        return jnp.stack([jnp.asarray(v, jnp.int32) for v in values])

    na, _, nq = block_factor.shape
    block = block_factor.reshape(2, na // 2, 2, nc // 2, nq).transpose(0, 2, 1, 4, 3)
    block = jnp.broadcast_to(block[:, None, None], (2, 4, 2, 2, na // 2, nq, nc // 2))
    block = lax.all_to_all(
        block.reshape(32, na // 2, nq, nc // 2), ("core", "x", "z"), 0, 0, tiled=True
    )
    block = block.transpose(1, 0, 2, 3).reshape(na // 2, 32 * nq, nc // 2)

    flat = amplitudes.reshape(ni * nj, nd, nc)
    own = [
        lax.ppermute(
            lax.dynamic_slice_in_dim(flat, (half ^ alpha) * (nc // 2), nc // 2, 2).transpose(
                1, 0, 2
            ),
            ("core", "z"),
            amplitude_route(alpha),
        )
        for alpha in range(2)
    ]
    own = turn(scalars(half), *own)

    low, high = own
    left_low, right_high = ring(low, "x", 1), ring(high, "x", -1)
    left_high, right_low = ring(high, "x", 1), ring(low, "x", -1)
    blocks = [block] + [ring(block, "y", k) for k in (1, 3, 2)]
    turned = pair_factor.transpose(1, 0, 2)
    turned, *own = lax.optimization_barrier((turned, *own))
    pair = [lax.ppermute(turned, ("core", "z"), amplitude_route(alpha)) for alpha in range(2)]
    before, after = ring(cycle_matrix, "y", 1), ring(cycle_matrix, "y", -1)
    far = [ring(left_low, "x", 1), ring(right_high, "x", -1)]
    pair += [sibling(v) for v in pair]
    amps = []
    for v in (*own, left_low, left_high, right_low, right_high):
        amps += [v, sibling(v)]
    for v in far:
        amps += [v, sibling(v)]

    w = form_integrals(scalars(y), pair, blocks)

    spots = scalars(x, (x + 3) % 4, (x + 1) % 4, (x + 2) % 4, core, 2 * core + half)
    parts = partial_ladder(spots, amps, w)
    parts = parts.reshape(32, -1, parts.shape[-1])
    parts = lax.all_to_all(parts, ("y", "core", "z"), 0, 0, tiled=True)
    direct, holes = settle(parts.reshape(4, 2, 4, -1, parts.shape[-1]))
    holes = lax.all_to_all(holes.reshape(16, nj, 16, 128), VIR, 0, 0, tiled=True)

    mid = cycle_matrix.shape[0] // 2
    matrix = []
    ends = ring(before[:mid], "y", 1), ring(after[mid:], "y", -1)
    for v in (cycle_matrix, before, after, *ends):
        matrix += [v, sibling(v)]

    occ_rows = nj // 8
    cols = virt_energy.shape[0] // 16
    occ_here = lax.dynamic_slice_in_dim(occ_energy, (2 * y + core) * occ_rows, occ_rows, 0)
    virt_here = lax.dynamic_slice_in_dim(virt_energy, (4 * x + z) * cols, cols, 0)
    row = (block_energy[None, :] - occ_here[:, None]).reshape(-1, 1)
    col = (virt_here[:, None] - occ_energy[None, :]).reshape(1, -1)
    return finish(scalars(y, core), holes, matrix, direct, row, col)


def solution(mesh):
    fine = jax.sharding.Mesh(mesh.devices.reshape(4, 2, 4, 4), ("y", "core", "x", "z"))
    return jax.shard_map(
        update,
        mesh=fine,
        in_specs=(
            P(VIR, None, OCC, None),
            P(VIR, OCC, None),
            P(None, None, OCC + VIR),
            P(OCC, VIR),
            P(),
            P(),
            P(),
        ),
        out_specs=P(OCC, VIR),
        check_vma=False,
    )
```

```python
import jax
import jax.numpy as jnp
from jax import lax
from jax.experimental import pallas as pl
from jax.experimental.pallas import tpu as pltpu
from jax.sharding import PartitionSpec as P


BF16, F32 = jnp.bfloat16, jnp.float32
OCC, VIR = ("y", "core"), ("x", "z")
ALL_CZ = [(c, z) for c in range(2) for z in range(4)]


def amplitude_route(alpha):
    return [(c * 4 + z, (z // 2) * 4 + 2 * c + ((z % 2) ^ alpha)) for c, z in ALL_CZ]


def ring(value, axis, shift):
    n = lax.axis_size(axis)
    return lax.ppermute(value, axis, [(i, (i + shift) % n) for i in range(n)])


def sibling(value):
    return lax.ppermute(value, "core", [(0, 1), (1, 0)])


def integrals_kernel(where_ref, *refs):
    pairs, blocks, out_ref, rhs = refs[:4], refs[4:8], refs[8], refs[9]
    nd, nb, naux = pairs[0].shape
    two, nq, nc = blocks[0].shape
    for far, ref in zip((0, 1, 3, 2), blocks):
        start = pl.multiple_of(((where_ref[0] + 4 - far) % 4) * nq, nq)
        for k in range(two):
            rhs[pl.ds(start, nq), k * nc : (k + 1) * nc] = ref[k]
    for s, ref in enumerate(pairs):
        got = jnp.dot(
            ref[...].reshape(nd * nb, naux), rhs[...], preferred_element_type=F32
        ).astype(BF16)
        for k in range(two):
            for d in range(nd):
                out_ref[(k * 4 + s) * nb : (k * 4 + s + 1) * nb, d * nc : (d + 1) * nc] = got[
                    d * nb : (d + 1) * nb, k * nc : (k + 1) * nc
                ]


def form_integrals(where, pairs, blocks):
    nd, nb, naux = pairs[0].shape
    na, nq, nc = blocks[0].shape
    step = 2
    return pl.pallas_call(
        integrals_kernel,
        grid_spec=pltpu.PrefetchScalarGridSpec(
            num_scalar_prefetch=1,
            grid=(na // step,),
            in_specs=[pl.BlockSpec((nd, nb, naux), lambda g, w: (0, 0, 0))] * 4
            + [pl.BlockSpec((step, nq, nc), lambda g, w: (g, 0, 0))] * 4,
            out_specs=pl.BlockSpec((step * 4 * nb, nd * nc), lambda g, w: (g, 0)),
            scratch_shapes=[pltpu.VMEM((naux, step * nc), BF16)],
        ),
        out_shape=jax.ShapeDtypeStruct((na * 4 * nb, nd * nc), BF16),
        cost_estimate=pl.CostEstimate(
            flops=8 * nd * nb * naux * na * nc, bytes_accessed=12 << 20, transcendentals=0
        ),
        name="integrals",
    )(where, *pairs, *blocks)


def turn_kernel(where_ref, zero_ref, one_ref, *out_refs):
    nd, _, nc = zero_ref.shape
    flip = where_ref[0] == 1
    for d in range(nd):
        p, q = zero_ref[d], one_ref[d]
        pair = jnp.concatenate([jnp.where(flip, q, p), jnp.where(flip, p, q)], axis=0)
        at = d % (nd // 2) * nc
        out_refs[d // (nd // 2)][at : at + nc, :] = pair.T


def turn(where, zero, one):
    nd, rows, nc = zero.shape
    return pl.pallas_call(
        turn_kernel,
        in_specs=[pl.BlockSpec(memory_space=pltpu.SMEM)]
        + [pl.BlockSpec(memory_space=pltpu.VMEM)] * 2,
        out_specs=[pl.BlockSpec(memory_space=pltpu.VMEM)] * 2,
        out_shape=[jax.ShapeDtypeStruct((nd * nc // 2, 2 * rows), BF16)] * 2,
        name="turn",
    )(where, zero, one)


def ladder_kernel(where_ref, *refs):
    amps, w_ref, out_ref, turned, sems = refs[:16], refs[16], refs[17], refs[18], refs[19]
    depth, wide = amps[0].shape
    g = pl.program_id(0)

    def load(n):
        chunk, part, side = n // 4, n // 2 % 2, n % 2
        spot = turned.at[pl.ds(part * depth, depth), pl.ds((2 * chunk + side) * wide, wide)]
        return pltpu.make_async_copy(amps[n], spot, sems.at[n])

    @pl.when(g == 0)
    def _():
        for n in range(16):
            load(n).start()

    _, _, nz, na, nb, _ = out_ref.shape
    for part in range(2):

        @pl.when(g == 0)
        def _():
            for n in range(8 * part, 8 * part + 8):
                load(n).wait()

        got = jnp.dot(
            w_ref[...],
            turned[:, 4 * part * wide : 4 * (part + 1) * wide],
            preferred_element_type=F32,
        ).astype(BF16)
        for n in range(4):
            y = where_ref[2 * part + n // 2]
            c = where_ref[4] ^ (n % 2)
            for s in range(nz):
                for a in range(na):
                    row = (a * nz + s) * nb
                    out_ref[y, c, where_ref[5] ^ s, a] = got[
                        row : row + nb, n * wide : (n + 1) * wide
                    ]


def partial_ladder(where, amps, w):
    wide = amps[0].shape[1]
    nrow, depth = w.shape
    step, nz, nb = 512, 4, 16
    na = step // (nz * nb)
    return pl.pallas_call(
        ladder_kernel,
        grid_spec=pltpu.PrefetchScalarGridSpec(
            num_scalar_prefetch=1,
            grid=(nrow // step,),
            in_specs=[pl.BlockSpec(memory_space=pl.ANY) for _ in amps]
            + [pl.BlockSpec((step, depth), lambda g, h: (g, 0))],
            out_specs=pl.BlockSpec((4, 2, nz, na, nb, wide), lambda g, h: (0, 0, 0, g, 0, 0)),
            scratch_shapes=[
                pltpu.VMEM((depth, 8 * wide), BF16),
                pltpu.SemaphoreType.DMA((len(amps),)),
            ],
        ),
        out_shape=jax.ShapeDtypeStruct((4, 2, nz, nrow // (nz * nb), nb, wide), BF16),
        cost_estimate=pl.CostEstimate(
            flops=16 * nrow * depth * wide, bytes_accessed=18 << 20, transcendentals=0
        ),
        name="ladder",
    )(where, *amps, w)


def settle_kernel(parts_ref, direct_ref, holes_ref, total, swapped):
    ny, two, nz, part, wide = parts_ref.shape
    rows = two * part
    nb = 16
    na = rows // nb
    ni = wide // na
    nj = wide // ni
    for h in range(two):
        acc = parts_ref[0, h, 0].astype(F32)
        for p in range(1, ny * nz):
            acc = acc + parts_ref[p // nz, h, p % nz].astype(F32)
        total[h * part : (h + 1) * part] = acc
    per = wide // nj
    for group in range(nb // per):
        blocks = [total[pl.ds(group * per + k, na, stride=nb), :] for k in range(per)]
        for i in range(ni):
            direct_ref[i * na : (i + 1) * na, group * wide : (group + 1) * wide] = jnp.concatenate(
                [m[:, i * nj : (i + 1) * nj] for m in blocks], axis=1
            )
        for k, m in enumerate(blocks):
            flipped = m.T
            swapped[pl.ds(group * per + k, nj, stride=nb), :] = jnp.concatenate(
                [flipped[i * nj : (i + 1) * nj, :] for i in range(ni)], axis=1
            )
    holes_ref[...] = swapped[...].astype(BF16)


def settle(parts):
    rows, wide = parts.shape[1] * parts.shape[3], parts.shape[4]
    return pl.pallas_call(
        settle_kernel,
        out_shape=(
            jax.ShapeDtypeStruct((128, 512), F32),
            jax.ShapeDtypeStruct((rows, wide), BF16),
        ),
        scratch_shapes=[pltpu.VMEM((rows, wide), F32), pltpu.VMEM((rows, wide), F32)],
        name="settle",
    )(parts)


def cycle_kernel(where_ref, *refs):
    holes, pieces, direct_ref = refs[:4], refs[4:20], refs[20]
    outs, held, lhs = refs[21:25], refs[25], refs[26]
    _, nb, wide = holes[0].shape
    deep = 4 * 4 * nb
    for far, ref in enumerate(holes):
        start = pl.multiple_of((where_ref[2] + 4 - far) % 4 * nb, nb)
        held[:, pl.ds(start, nb), :] = ref[...]
    for n in range(8):
        owner = (where_ref[0] + SHIFTS[n // 2]) % 4 * 2 + (where_ref[1] ^ (n % 2))
        block = held[pl.ds(owner * 4, 4)].reshape(deep, wide)
        lhs[:, n * deep : (n + 1) * deep] = block.T
    for column in range(4):
        acc = None
        for n in range(8):
            ref = pieces[n // 2 * 4 + column // 2 * 2 + n % 2]
            row = column % 2 * deep
            got = jnp.dot(
                lhs[:, n * deep : (n + 1) * deep],
                ref[row : row + deep, :],
                preferred_element_type=F32,
            )
            acc = got if acc is None else acc + got
        if column == 0:
            outs[0][...] = direct_ref[...] + acc
        else:
            outs[column][...] = acc.astype(BF16)


SHIFTS = (0, 3, 1, 2)


def partial_cycle(where, holes, pieces, direct):
    nk, nb, wide = holes[0].shape
    return pl.pallas_call(
        cycle_kernel,
        in_specs=[pl.BlockSpec(memory_space=pltpu.SMEM)]
        + [pl.BlockSpec(memory_space=pltpu.VMEM)] * (len(pieces) + 5),
        out_specs=[pl.BlockSpec(memory_space=pltpu.VMEM)] * 4,
        out_shape=[jax.ShapeDtypeStruct(direct.shape, F32)]
        + [jax.ShapeDtypeStruct(direct.shape, BF16)] * 3,
        scratch_shapes=[
            pltpu.VMEM((nk, 4 * nb, wide), BF16),
            pltpu.VMEM((wide, 8 * 16 * nb), BF16),
        ],
        name="cycle",
    )(where, *holes, *pieces, direct)


def update(
    amplitudes, pair_factor, block_factor, cycle_matrix, occ_energy, block_energy, virt_energy
):
    y, core, x, z = (lax.axis_index(n) for n in ("y", "core", "x", "z"))
    half = z % 2
    ni, nj, nd, nc = amplitudes.shape

    def scalars(*values):
        return jnp.stack([jnp.asarray(v, jnp.int32) for v in values])

    na, _, nq = block_factor.shape
    block = block_factor.reshape(2, na // 2, 2, nc // 2, nq).transpose(0, 2, 1, 4, 3)
    block = jnp.broadcast_to(block[:, None, None], (2, 4, 2, 2, na // 2, nq, nc // 2))
    block = lax.all_to_all(
        block.reshape(32, na // 2, nq, nc // 2), ("core", "x", "z"), 0, 0, tiled=True
    )
    block = block.transpose(1, 0, 2, 3).reshape(na // 2, 32 * nq, nc // 2)

    flat = amplitudes.reshape(ni * nj, nd, nc)
    own = [
        lax.ppermute(
            lax.dynamic_slice_in_dim(flat, (half ^ alpha) * (nc // 2), nc // 2, 2).transpose(
                1, 0, 2
            ),
            ("core", "z"),
            amplitude_route(alpha),
        )
        for alpha in range(2)
    ]
    own = turn(scalars(half), *own)

    grid = cycle_matrix.reshape(nj // 8, 4, -1, cycle_matrix.shape[1])
    mixed = []
    for k in range(4):
        v = lax.dynamic_index_in_dim(grid, (x + k) % 4, 1, keepdims=False)
        v = v.reshape(-1, grid.shape[3])
        mixed.append(ring(v, "x", k) if k else v)
    base = [jnp.concatenate(mixed[:2]), jnp.concatenate(mixed[2:])]
    base, own = lax.optimization_barrier((base, own))

    low, high = own
    left_low, right_high = ring(low, "x", 1), ring(high, "x", -1)
    left_high, right_low = ring(high, "x", 1), ring(low, "x", -1)
    blocks = [block] + [ring(block, "y", k) for k in (1, 3, 2)]
    turned = pair_factor.transpose(1, 0, 2)
    turned, *own = lax.optimization_barrier((turned, *own))
    pair = [lax.ppermute(turned, ("core", "z"), amplitude_route(alpha)) for alpha in range(2)]
    before, after = [ring(base[0], "y", 1)], [ring(base[1], "y", -1)]
    before.append(ring(base[1], "y", 1))
    after.insert(0, ring(base[0], "y", -1))
    far = [ring(left_low, "x", 1), ring(right_high, "x", -1)]
    pair += [sibling(v) for v in pair]
    amps = []
    for v in (*own, left_low, left_high, right_low, right_high):
        amps += [v, sibling(v)]
    for v in far:
        amps += [v, sibling(v)]

    ends = [ring(before[0], "y", 1), ring(after[1], "y", -1)]

    w = form_integrals(scalars(y), pair, blocks)

    spots = scalars(x, (x + 3) % 4, (x + 1) % 4, (x + 2) % 4, core, 2 * core + half)
    parts = partial_ladder(spots, amps, w)
    parts = parts.reshape(32, -1, parts.shape[-1])
    parts = lax.all_to_all(parts, ("y", "core", "z"), 0, 0, tiled=True)
    matrix = []
    for v in (*base, *before, *after, *ends):
        matrix += [v, sibling(v)]
    direct, holes = settle(parts.reshape(4, 2, 4, -1, parts.shape[-1]))
    holes = holes.reshape(nj, -1, holes.shape[1])
    holes = [holes] + [ring(holes, "z", k) for k in (1, 2, 3)]

    occ_rows = nj // 8
    cols = virt_energy.shape[0] // 16
    occ_here = lax.dynamic_slice_in_dim(occ_energy, (2 * y + core) * occ_rows, occ_rows, 0)
    virt_here = lax.dynamic_slice_in_dim(virt_energy, (4 * x + z) * cols, cols, 0)
    row = (block_energy[None, :] - occ_here[:, None]).reshape(-1, 1)
    col = (virt_here[:, None] - occ_energy[None, :]).reshape(1, -1)
    total, *sums = partial_cycle(scalars(y, core, z), holes, matrix, direct)
    for k, v in enumerate(sums):
        total = total + ring(v, "x", -k - 1).astype(F32)
    return total / (row + col)


def solution(mesh):
    fine = jax.sharding.Mesh(mesh.devices.reshape(4, 2, 4, 4), ("y", "core", "x", "z"))
    return jax.shard_map(
        update,
        mesh=fine,
        in_specs=(
            P(VIR, None, OCC, None),
            P(VIR, OCC, None),
            P(None, None, OCC + VIR),
            P(OCC, VIR),
            P(),
            P(),
            P(),
        ),
        out_specs=P(OCC, VIR),
        check_vma=False,
    )
```

```python
import jax
import jax.numpy as jnp
from jax import lax
from jax.experimental import pallas as pl
from jax.experimental.pallas import tpu as pltpu
from jax.sharding import PartitionSpec as P


BF16, F32 = jnp.bfloat16, jnp.float32
OCC, VIR = ("y", "core"), ("x", "z")
ALL_CZ = [(c, z) for c in range(2) for z in range(4)]


def amplitude_route(alpha):
    return [(c * 4 + z, (z // 2) * 4 + 2 * c + ((z % 2) ^ alpha)) for c, z in ALL_CZ]


def ring(value, axis, shift):
    n = lax.axis_size(axis)
    return lax.ppermute(value, axis, [(i, (i + shift) % n) for i in range(n)])


def sibling(value):
    return lax.ppermute(value, "core", [(0, 1), (1, 0)])


def integrals_kernel(where_ref, *refs):
    pairs, blocks, out_ref, rhs = refs[:4], refs[4:8], refs[8], refs[9]
    nd, nb, naux = pairs[0].shape
    two, nq, nc = blocks[0].shape
    for far, ref in zip((0, 1, 3, 2), blocks):
        start = pl.multiple_of(((where_ref[0] + 4 - far) % 4) * nq, nq)
        for k in range(two):
            rhs[pl.ds(start, nq), k * nc : (k + 1) * nc] = ref[k]
    for s, ref in enumerate(pairs):
        got = jnp.dot(
            ref[...].reshape(nd * nb, naux), rhs[...], preferred_element_type=F32
        ).astype(BF16)
        for k in range(two):
            for d in range(nd):
                out_ref[(k * 4 + s) * nb : (k * 4 + s + 1) * nb, d * nc : (d + 1) * nc] = got[
                    d * nb : (d + 1) * nb, k * nc : (k + 1) * nc
                ]


def form_integrals(where, pairs, blocks):
    nd, nb, naux = pairs[0].shape
    na, nq, nc = blocks[0].shape
    step = 2
    return pl.pallas_call(
        integrals_kernel,
        grid_spec=pltpu.PrefetchScalarGridSpec(
            num_scalar_prefetch=1,
            grid=(na // step,),
            in_specs=[pl.BlockSpec((nd, nb, naux), lambda g, w: (0, 0, 0))] * 4
            + [pl.BlockSpec((step, nq, nc), lambda g, w: (g, 0, 0))] * 4,
            out_specs=pl.BlockSpec((step * 4 * nb, nd * nc), lambda g, w: (g, 0)),
            scratch_shapes=[pltpu.VMEM((naux, step * nc), BF16)],
        ),
        out_shape=jax.ShapeDtypeStruct((na * 4 * nb, nd * nc), BF16),
        cost_estimate=pl.CostEstimate(
            flops=8 * nd * nb * naux * na * nc, bytes_accessed=12 << 20, transcendentals=0
        ),
        name="integrals",
    )(where, *pairs, *blocks)


def turn_kernel(where_ref, zero_ref, one_ref, *out_refs):
    nd, _, nc = zero_ref.shape
    flip = where_ref[0] == 1
    for d in range(nd):
        p, q = zero_ref[d], one_ref[d]
        pair = jnp.concatenate([jnp.where(flip, q, p), jnp.where(flip, p, q)], axis=0)
        at = d % (nd // 2) * nc
        out_refs[d // (nd // 2)][at : at + nc, :] = pair.T


def turn(where, zero, one):
    nd, rows, nc = zero.shape
    return pl.pallas_call(
        turn_kernel,
        in_specs=[pl.BlockSpec(memory_space=pltpu.SMEM)]
        + [pl.BlockSpec(memory_space=pltpu.VMEM)] * 2,
        out_specs=[pl.BlockSpec(memory_space=pltpu.VMEM)] * 2,
        out_shape=[jax.ShapeDtypeStruct((nd * nc // 2, 2 * rows), BF16)] * 2,
        name="turn",
    )(where, zero, one)


def ladder_kernel(where_ref, *refs):
    amps, w_ref, out_ref, turned, sems = refs[:16], refs[16], refs[17], refs[18], refs[19]
    depth, wide = amps[0].shape
    g = pl.program_id(0)

    def load(n):
        chunk, part, side = n // 4, n // 2 % 2, n % 2
        spot = turned.at[pl.ds(part * depth, depth), pl.ds((2 * chunk + side) * wide, wide)]
        return pltpu.make_async_copy(amps[n], spot, sems.at[n])

    @pl.when(g == 0)
    def _():
        for n in range(16):
            load(n).start()

    _, _, nz, na, nb, _ = out_ref.shape

    def product(begin, count):
        got = jnp.dot(
            w_ref[...],
            turned[:, begin * wide : (begin + count) * wide],
            preferred_element_type=F32,
        ).astype(BF16)
        for n in range(count):
            y = where_ref[(begin + n) // 2]
            c = where_ref[4] ^ (n % 2)
            for s in range(nz):
                for a in range(na):
                    row = (a * nz + s) * nb
                    out_ref[y, c, where_ref[5] ^ s, a] = got[
                        row : row + nb, n * wide : (n + 1) * wide
                    ]

    @pl.when(g == 0)
    def _():
        for part in range(2):
            for n in range(8 * part, 8 * part + 8):
                load(n).wait()
            product(4 * part, 4)

    @pl.when(g > 0)
    def _():
        product(0, 8)


def partial_ladder(where, amps, w):
    wide = amps[0].shape[1]
    nrow, depth = w.shape
    step, nz, nb = 256, 4, 16
    na = step // (nz * nb)
    return pl.pallas_call(
        ladder_kernel,
        grid_spec=pltpu.PrefetchScalarGridSpec(
            num_scalar_prefetch=1,
            grid=(nrow // step,),
            in_specs=[pl.BlockSpec(memory_space=pl.ANY) for _ in amps]
            + [pl.BlockSpec((step, depth), lambda g, h: (g, 0))],
            out_specs=pl.BlockSpec((4, 2, nz, na, nb, wide), lambda g, h: (0, 0, 0, g, 0, 0)),
            scratch_shapes=[
                pltpu.VMEM((depth, 8 * wide), BF16),
                pltpu.SemaphoreType.DMA((len(amps),)),
            ],
        ),
        out_shape=jax.ShapeDtypeStruct((4, 2, nz, nrow // (nz * nb), nb, wide), BF16),
        cost_estimate=pl.CostEstimate(
            flops=16 * nrow * depth * wide, bytes_accessed=18 << 20, transcendentals=0
        ),
        name="ladder",
    )(where, *amps, w)


def settle_kernel(parts_ref, direct_ref, holes_ref, total, swapped):
    ny, two, nz, part, wide = parts_ref.shape
    rows = two * part
    nb = 16
    na = rows // nb
    ni = wide // na
    nj = wide // ni
    for h in range(two):
        acc = parts_ref[0, h, 0].astype(F32)
        for p in range(1, ny * nz):
            acc = acc + parts_ref[p // nz, h, p % nz].astype(F32)
        total[h * part : (h + 1) * part] = acc
    per = wide // nj
    for group in range(nb // per):
        blocks = [total[pl.ds(group * per + k, na, stride=nb), :] for k in range(per)]
        for i in range(ni):
            direct_ref[i * na : (i + 1) * na, group * wide : (group + 1) * wide] = jnp.concatenate(
                [m[:, i * nj : (i + 1) * nj] for m in blocks], axis=1
            )
        for k, m in enumerate(blocks):
            flipped = m.T
            swapped[pl.ds(group * per + k, nj, stride=nb), :] = jnp.concatenate(
                [flipped[i * nj : (i + 1) * nj, :] for i in range(ni)], axis=1
            )
    holes_ref[...] = swapped[...].astype(BF16)


def settle(parts):
    rows, wide = parts.shape[1] * parts.shape[3], parts.shape[4]
    return pl.pallas_call(
        settle_kernel,
        out_shape=(
            jax.ShapeDtypeStruct((128, 512), F32),
            jax.ShapeDtypeStruct((rows, wide), BF16),
        ),
        scratch_shapes=[pltpu.VMEM((rows, wide), F32), pltpu.VMEM((rows, wide), F32)],
        name="settle",
    )(parts)


def cycle_kernel(where_ref, *refs):
    holes, pieces, direct_ref = refs[:4], refs[4:20], refs[20]
    outs, held, lhs = refs[21:25], refs[25], refs[26]
    _, nb, wide = holes[0].shape
    deep = 4 * 4 * nb
    for far, ref in enumerate(holes):
        start = pl.multiple_of((where_ref[2] + 4 - far) % 4 * nb, nb)
        held[:, pl.ds(start, nb), :] = ref[...]
    for n in range(8):
        owner = (where_ref[0] + SHIFTS[n // 2]) % 4 * 2 + (where_ref[1] ^ (n % 2))
        block = held[pl.ds(owner * 4, 4)].reshape(deep, wide)
        lhs[:, n * deep : (n + 1) * deep] = block.T
    for column in range(4):
        acc = None
        for n in range(8):
            ref = pieces[n // 2 * 4 + column // 2 * 2 + n % 2]
            row = column % 2 * deep
            got = jnp.dot(
                lhs[:, n * deep : (n + 1) * deep],
                ref[row : row + deep, :],
                preferred_element_type=F32,
            )
            acc = got if acc is None else acc + got
        if column == 0:
            outs[0][...] = direct_ref[...] + acc
        else:
            outs[column][...] = acc.astype(BF16)


SHIFTS = (0, 3, 1, 2)


def partial_cycle(where, holes, pieces, direct):
    nk, nb, wide = holes[0].shape
    return pl.pallas_call(
        cycle_kernel,
        in_specs=[pl.BlockSpec(memory_space=pltpu.SMEM)]
        + [pl.BlockSpec(memory_space=pltpu.VMEM)] * (len(pieces) + 5),
        out_specs=[pl.BlockSpec(memory_space=pltpu.VMEM)] * 4,
        out_shape=[jax.ShapeDtypeStruct(direct.shape, F32)]
        + [jax.ShapeDtypeStruct(direct.shape, BF16)] * 3,
        scratch_shapes=[
            pltpu.VMEM((nk, 4 * nb, wide), BF16),
            pltpu.VMEM((wide, 8 * 16 * nb), BF16),
        ],
        name="cycle",
    )(where, *holes, *pieces, direct)


def update(
    amplitudes, pair_factor, block_factor, cycle_matrix, occ_energy, block_energy, virt_energy
):
    y, core, x, z = (lax.axis_index(n) for n in ("y", "core", "x", "z"))
    half = z % 2
    ni, nj, nd, nc = amplitudes.shape

    def scalars(*values):
        return jnp.stack([jnp.asarray(v, jnp.int32) for v in values])

    na, _, nq = block_factor.shape
    block = block_factor.reshape(2, na // 2, 2, nc // 2, nq).transpose(0, 2, 1, 4, 3)
    block = jnp.broadcast_to(block[:, None, None], (2, 4, 2, 2, na // 2, nq, nc // 2))
    block = lax.all_to_all(
        block.reshape(32, na // 2, nq, nc // 2), ("core", "x", "z"), 0, 0, tiled=True
    )

    flat = amplitudes.reshape(ni * nj, nd, nc)
    own = [
        lax.ppermute(
            lax.dynamic_slice_in_dim(flat, (half ^ alpha) * (nc // 2), nc // 2, 2).transpose(
                1, 0, 2
            ),
            ("core", "z"),
            amplitude_route(alpha),
        )
        for alpha in range(2)
    ]
    own = turn(scalars(half), *own)

    grid = cycle_matrix.reshape(nj // 8, 4, -1, cycle_matrix.shape[1])
    mixed = []
    for k in range(4):
        v = lax.dynamic_index_in_dim(grid, (x + k) % 4, 1, keepdims=False)
        v = v.reshape(-1, grid.shape[3])
        mixed.append(ring(v, "x", k) if k else v)
    base = [jnp.concatenate(mixed[:2]), jnp.concatenate(mixed[2:])]
    base, own = lax.optimization_barrier((base, own))

    low, high = own
    left_low, right_high = ring(low, "x", 1), ring(high, "x", -1)
    left_high, right_low = ring(high, "x", 1), ring(low, "x", -1)
    block, _ = lax.optimization_barrier((block, low))
    block = block.transpose(1, 0, 2, 3).reshape(na // 2, 32 * nq, nc // 2)
    blocks = [block] + [ring(block, "y", k) for k in (1, 3, 2)]
    turned = pair_factor.transpose(1, 0, 2)
    turned, *own = lax.optimization_barrier((turned, *own))
    pair = [lax.ppermute(turned, ("core", "z"), amplitude_route(alpha)) for alpha in range(2)]
    before, after = [ring(base[0], "y", 1)], [ring(base[1], "y", -1)]
    before.append(ring(base[1], "y", 1))
    after.insert(0, ring(base[0], "y", -1))
    far = [ring(left_low, "x", 1), ring(right_high, "x", -1)]
    pair += [sibling(v) for v in pair]
    amps = []
    for v in (*own, left_low, left_high, right_low, right_high):
        amps += [v, sibling(v)]
    for v in far:
        amps += [v, sibling(v)]

    ends = [ring(before[0], "y", 1), ring(after[1], "y", -1)]

    w = form_integrals(scalars(y), pair, blocks)

    spots = scalars(x, (x + 3) % 4, (x + 1) % 4, (x + 2) % 4, core, 2 * core + half)
    parts = partial_ladder(spots, amps, w)
    parts = parts.reshape(32, -1, parts.shape[-1])
    parts = lax.all_to_all(parts, ("y", "core", "z"), 0, 0, tiled=True)
    matrix = []
    for v in (*base, *before, *after, *ends):
        matrix += [v, sibling(v)]
    direct, holes = settle(parts.reshape(4, 2, 4, -1, parts.shape[-1]))
    holes = holes.reshape(nj, -1, holes.shape[1])
    holes = [holes] + [ring(holes, "z", k) for k in (1, 2, 3)]

    occ_rows = nj // 8
    cols = virt_energy.shape[0] // 16
    occ_here = lax.dynamic_slice_in_dim(occ_energy, (2 * y + core) * occ_rows, occ_rows, 0)
    virt_here = lax.dynamic_slice_in_dim(virt_energy, (4 * x + z) * cols, cols, 0)
    row = (block_energy[None, :] - occ_here[:, None]).reshape(-1, 1)
    col = (virt_here[:, None] - occ_energy[None, :]).reshape(1, -1)
    total, *sums = partial_cycle(scalars(y, core, z), holes, matrix, direct)
    for k, v in enumerate(sums):
        total = total + ring(v, "x", -k - 1).astype(F32)
    return total / (row + col)


def solution(mesh):
    fine = jax.sharding.Mesh(mesh.devices.reshape(4, 2, 4, 4), ("y", "core", "x", "z"))
    return jax.shard_map(
        update,
        mesh=fine,
        in_specs=(
            P(VIR, None, OCC, None),
            P(VIR, OCC, None),
            P(None, None, OCC + VIR),
            P(OCC, VIR),
            P(),
            P(),
            P(),
        ),
        out_specs=P(OCC, VIR),
        check_vma=False,
    )
```
